32 devices in a mesh: tok: 16 (over z, y, core), col: 2 (over x).
Axes of the slice: x: 2, y: 2, z: 4, core: 2. Of those that a mesh axis runs over, the one named last changes fastest.
Arguments:
- hidden: bfloat16 [4096, 8192], P('tok'), may hold values from -6 to 6
- norm_gain: float32 [8192], replicated, may hold values from 0.1 to 1.9
- token_ids: int32 [4096], P('tok'), may hold values from 0 to 128000, as said below
- owner: int32 [1], replicated, may hold values from 0 to 15
- query_store: bfloat16 [16, 8192, 4096], P('tok', None, 'col'), may hold values from -0.0625 to 0.0625
- key_store: bfloat16 [16, 8192, 512], P('tok', None, 'col'), may hold values from -0.0625 to 0.0625
Outputs:
- queries: bfloat16 [4096, 4096], P('tok', 'col')
- keys: bfloat16 [4096, 512], P('tok', 'col')
- hessian: float32 [8192, 8192], P('col', 'tok')
The draws below stay inside these ranges and needn't reach their ends.
Inputs may be any that keep to these rules, and one draw needn't show every extreme that they name: `token_ids`: id 128000 marks the first token of a document; every other id is below it.
All inputs are finite; a program needn't handle non-finite values.
Results may differ from the reference program's by a relative error of at most 0.0049.
Values may be sent and summed in bfloat16 or wider, within the bound.
A program may use at most 256 MiB of HBM per device.

```python
import jax
import jax.numpy as jnp
from jax import lax

D = 8192
HEAD = 128
SEQ = 128
QCOLS = 4096
KCOLS = 512
TOKENS = 4096
LAYERS = 16
N_TOK = 16


def draw_token_ids(key, part):
    base = jax.random.fold_in(key, 11)
    first_key, second_key = jax.random.split(base)
    marks = jax.random.randint(first_key, (TOKENS,), 0, 32) == 0
    words = jax.random.randint(second_key, (TOKENS,), 0, 128000)
    return jnp.where(marks, 128000, words).astype(jnp.int32)


def block_levels(rng, shape, shards, least, high):
    loudness, own = 1.0, jax.random.fold_in(rng, 6)
    for axis_at, blocks in shards:
        heights = jnp.exp(jax.random.uniform(jax.random.fold_in(own, axis_at), (blocks,), jnp.float32, least / len(shards), high / len(shards)))
        loudness = loudness * jnp.repeat(heights, shape[axis_at] // blocks).reshape([-1 if axis == axis_at else 1 for axis in range(len(shape))])
    return loudness


def normal_values(stream_key, extent, scale, reach, cuts=(), kind=jnp.bfloat16):
    array = scale * jax.random.normal(stream_key, extent, jnp.float32)
    if cuts:
        array = array * block_levels(stream_key, extent, cuts, -0.22, 0.18)
    return jnp.clip(array, -reach, reach).astype(kind)


def setup_inputs(seed: int = 0) -> dict:
    splits = jax.random.split(jax.random.key(seed), 7)
    return {
        "hidden": normal_values(splits[0], (TOKENS, D), 1.0, 6.0, ((0, 16),)),
        "norm_gain": jnp.clip(1.0 + 0.18 * jax.random.normal(splits[1], (D,), jnp.float32), 0.1, 1.9),
        "token_ids": draw_token_ids(jax.random.fold_in(splits[6], 71), 0),
        "owner": jax.random.randint(splits[3], (1,), 0, N_TOK).astype(jnp.int32),
        "query_store": normal_values(splits[4], (LAYERS, D, QCOLS), D ** -0.5, 0.0625, ((0, 16), (2, 2))),
        "key_store": normal_values(splits[5], (LAYERS, D, KCOLS), D ** -0.5, 0.0625, ((0, 16), (2, 2))),
    }


begin_token = 128000
rope_base = 500000.0

def positions(token_ids):
    samples = token_ids.reshape(-1, SEQ)
    index = jnp.arange(SEQ, dtype=jnp.int32)
    starts = jnp.where(samples == begin_token, index[None, :], jnp.zeros_like(samples))
    latest = lax.cummax(starts, axis=1)
    return (index[None, :] - latest).reshape(-1)

def rotate(values, place, start):
    width = values.shape[1]
    dims = (start + jnp.arange(width, dtype=jnp.int32)) % HEAD
    pair = (dims[0::2] // 2).astype(jnp.float32)
    freq = jnp.power(jnp.float32(rope_base), -2.0 * pair / HEAD)
    angle = place.astype(jnp.float32)[:, None] * freq[None, :]
    cosine = jnp.cos(angle)
    sine = jnp.sin(angle)
    even = values[:, 0::2]
    odd = values[:, 1::2]
    first = even * cosine - odd * sine
    second = even * sine + odd * cosine
    return jnp.stack([first, second], axis=-1).reshape(values.shape[0], width)

def normalize(hidden, norm_gain):
    wide = hidden.astype(jnp.float32)
    meansq = lax.optimization_barrier(jnp.mean(wide * wide, axis=-1, keepdims=True))
    return (wide * lax.rsqrt(meansq + 1e-05) * norm_gain[None, :]).astype(jnp.bfloat16)

def reference(hidden, norm_gain, token_ids, owner, query_store, key_store):
    normed = normalize(hidden, norm_gain)
    place = positions(token_ids)
    slot = owner[0].astype(jnp.int32)
    weight_q = lax.dynamic_index_in_dim(query_store, slot, 0, keepdims=False)
    weight_k = lax.dynamic_index_in_dim(key_store, slot, 0, keepdims=False)
    raw_q = jnp.dot(normed, weight_q, preferred_element_type=jnp.float32)
    raw_k = jnp.dot(normed, weight_k, preferred_element_type=jnp.float32)
    queries = rotate(raw_q, place, 0).astype(jnp.bfloat16)
    keys = rotate(raw_k, place, 0).astype(jnp.bfloat16)
    gram = lax.dot_general(normed, normed, (((0,), (0,)), ((), ())), preferred_element_type=jnp.float32)
    hessian = gram * (2.0 / TOKENS)
    return (queries, keys, hessian)
```

```python
import functools

import jax
import jax.numpy as jnp
from jax import lax
from jax.experimental import pallas as pl
from jax.experimental.pallas import tpu as pltpu
from jax.sharding import PartitionSpec as P

HEAD = 128
SEQ = 128


begin_token = 128000
rope_base = 500000.0


def scatter_weights(query, key, owner):
    groups = lax.axis_size("tok")
    depth, width = query.shape
    piece = width // groups
    mine = lax.axis_index("tok") == owner
    query = jnp.moveaxis(query.reshape(depth, groups, piece), 1, 0)
    key = key.reshape(groups, depth * key.shape[1] // groups // piece, piece)
    both = jnp.concatenate([query, key], axis=1)
    return jnp.where(mine, both, jnp.zeros_like(both))


def positions(token_ids):
    samples = token_ids.reshape(-1, SEQ)
    index = jnp.arange(SEQ, dtype=jnp.int32)
    starts = jnp.where(samples == begin_token, index[None, :], jnp.zeros_like(samples))
    latest = lax.cummax(starts, axis=1)
    return (index[None, :] - latest).reshape(-1)


def rotate(values, place, start):
    width = values.shape[1]
    period = HEAD if width % HEAD == 0 else width
    dims = (start + jnp.arange(period, dtype=jnp.int32)) % HEAD
    pair = (dims // 2).astype(jnp.float32)
    freq = jnp.power(jnp.float32(rope_base), -2.0 * pair / HEAD)
    angle = place.astype(jnp.float32)[:, None] * freq[None, :]
    even = dims % 2 == 0
    sine = jnp.where(even[None, :], -jnp.sin(angle), jnp.sin(angle))
    cosine, sine = lax.optimization_barrier((jnp.cos(angle), sine))
    cosine = jnp.tile(cosine, (1, width // period))
    sine = jnp.tile(sine, (1, width // period))
    following = jnp.concatenate([values[:, 1:], values[:, :1]], axis=1)
    previous = jnp.concatenate([values[:, -1:], values[:, :-1]], axis=1)
    even = jnp.arange(width, dtype=jnp.int32) % 2 == 0
    other = jnp.where(even[None, :], following, previous)
    return values * cosine + other * sine


def normalize(hidden, norm_gain):
    wide = hidden.astype(jnp.float32)
    meansq = jnp.mean(wide * wide, axis=-1, keepdims=True)
    return (wide * lax.rsqrt(meansq + 1e-05) * norm_gain[None, :]).astype(jnp.bfloat16)


def transposed_product(left, right):
    return lax.dot_general(
        left, right, (((0,), (0,)), ((), ())), preferred_element_type=jnp.float32
    )


def shards(hidden, norm_gain, token_ids, owner, query_store, key_store):
    normed = normalize(hidden, norm_gain)
    place = positions(token_ids)
    column = lax.axis_index("col")
    row_width = normed.shape[1] // lax.axis_size("col")
    row_block = lax.dynamic_slice_in_dim(normed, column * row_width, row_width, 1)
    total_tokens = normed.shape[0] * lax.axis_size("tok")
    groups, parts = lax.axis_size("tok"), lax.axis_size("col")
    depth, q_width = query_store.shape[1:]
    k_width = key_store.shape[2]
    masked = scatter_weights(query_store[0], key_store[0], owner[0])
    gathered = lax.all_gather(row_block, "tok", axis=0, tiled=True)
    col_block = lax.all_to_all(normed, "tok", split_axis=1, concat_axis=0, tiled=True)
    masked, gathered = lax.optimization_barrier((masked, gathered))
    owned = lax.psum_scatter(masked, "tok", scatter_dimension=0, tiled=False)
    gram = transposed_product(gathered, col_block)
    hessian = gram * (2.0 / total_tokens)
    key_rows = owned[depth:].reshape(depth // groups, k_width)
    weight_k = lax.all_gather(key_rows, "tok", axis=0, tiled=True)
    weight_q = lax.all_to_all(owned[:depth], "col", split_axis=0, concat_axis=1, tiled=True)
    partial = jnp.dot(gathered, weight_q, preferred_element_type=jnp.float32).astype(jnp.bfloat16)
    partial = lax.all_to_all(partial, "col", split_axis=1, concat_axis=0, tiled=True)
    partial = partial.reshape(parts, total_tokens, q_width // groups).astype(jnp.float32)
    summed = jnp.sum(partial, axis=0).astype(jnp.bfloat16)
    raw_q = lax.all_to_all(summed, "tok", split_axis=0, concat_axis=1, tiled=True).astype(jnp.float32)
    raw_k = jnp.dot(normed, weight_k, preferred_element_type=jnp.float32)
    queries = rotate(raw_q, place, column * q_width).astype(jnp.bfloat16)
    keys = rotate(raw_k, place, column * k_width).astype(jnp.bfloat16)
    return (queries, keys, hessian)


MESH = pl.DeviceIdType.MESH

DEPTH, WIDE, CORES = 4, 2, 2
CHIPS = DEPTH * WIDE
CUT = 4
LAG = 2
BASE = 128
PACK = 4
ROUTES = (
    (
        (
            (8438017, 76075297, 135257917, 84529957, 59165977),
            (16892677, 46483213, 33803287, 0, 0),
            (25347337, 2321, 97208851, 6191, 0),
            (12664832, 8438017, 76075297, 46482439, 3095),
            (42256657, 25347337, 8438017, 114114560, 7223),
            (29575957, 50710543, 71844613, 16896547, 0),
            (59165977, 42256657, 4211977, 25346563, 0),
            (67620637, 29575957, 33800965, 3095, 1031),
        ),
        (
            (126803257, 118348597, 101439277, 109893937, 92984617),
            (4211461, 71844355, 16896547, 135257917, 0),
            (25347337, 4218169, 126796291, 118348597, 109893937),
            (33801997, 773, 76075297, 131023879, 8255),
            (42256657, 25347337, 8438017, 76075297, 126803257),
            (50711317, 12666637, 71845903, 16896547, 135257917),
            (0, 0, 0, 0, 0),
            (0, 0, 0, 0, 0),
        ),
        (
            (0, 0, 0, 0, 0),
            (0, 0, 0, 0, 0),
            (25347337, 59165977, 63392017, 42258463, 0),
            (33801997, 50711317, 25347337, 42256657, 67620637),
            (54937873, 42257947, 67620637, 33801997, 0),
            (50711317, 67620637, 59165977, 0, 0),
            (59165977, 67620637, 0, 0, 0),
            (67620637, 59165977, 0, 0, 0),
        ),
    ),
    (
        (
            (8438017, 42256657, 67620637, 50711317, 0),
            (29573120, 25347337, 59165977, 92984617, 2063),
            (25347337, 92984617, 84529957, 101439277, 0),
            (46483213, 12667927, 33801223, 0, 0),
            (42256657, 135257917, 8438017, 118348597, 0),
            (29575957, 21121039, 50710027, 88752128, 5675),
            (59165977, 29573120, 8438017, 21121039, 1547),
            (67620637, 50711317, 0, 16892677, 92984617),
        ),
        (
            (8438017, 0, 0, 0, 0),
            (16892677, 8438017, 0, 0, 0),
            (135257917, 8438017, 118348597, 126803257, 109893937),
            (33801997, 25347337, 16892677, 92984617, 0),
            (42256657, 4212493, 33800707, 25347337, 126803257),
            (50711317, 131025169, 12673087, 88753159, 42260011),
            (0, 0, 0, 0, 0),
            (0, 0, 0, 0, 0),
        ),
        (
            (0, 0, 0, 0, 0),
            (0, 0, 0, 0, 0),
            (38031649, 63392275, 46485535, 12667927, 76071943),
            (21120781, 54937099, 88755739, 33805867, 84529957),
            (42256657, 67620637, 59165977, 0, 0),
            (50711317, 59165977, 67620637, 42256657, 0),
            (63393049, 59166751, 0, 12664832, 1031),
            (54939421, 67620379, 0, 0, 0),
        ),
    ),
)


def step_entries(owner_at, direction, position):
    entries = []
    for number in ROUTES[owner_at][direction][position]:
        for _ in range(PACK):
            entries.append(number % BASE)
            number //= BASE
    return entries


def packed_table(owner_at, direction, arrivals):
    table = []
    for position in range(CHIPS):
        entries = None
        if not arrivals:
            entries = step_entries(owner_at, direction, position) + [0] * LAG
        else:
            z = position // WIDE + (0, -1, 1)[direction]
            sender = position ^ 1 if direction == 0 else z * WIDE + position % WIDE
            entries = [0] * LAG + (
                step_entries(owner_at, direction, sender) if 0 <= z < DEPTH else [0] * len(step_entries(owner_at, 0, 0))
            )
        entries += [0] * (-len(entries) % PACK)
        table.append([
            sum(entries[i + j] * BASE**j for j in range(PACK)) for i in range(0, len(entries), PACK)
        ])
    return table


def choose(index, options):
    value = jnp.int32(0)
    for at, option in enumerate(options):
        if isinstance(option, int) and option == 0:
            continue
        value = jnp.where(index == at, jnp.int32(option) if isinstance(option, int) else option, value)
    return value


def exchange_kernel(
    owner, x_ref, wq_ref, wk_ref, all_ref, cols_ref, slots_ref, other_ref,
    x_buf, w_buf, local_sem, recv_sem, send_sem, feed_sem, twin_send, twin_recv, cross_send, cross_recv,
):
    tok, col = lax.axis_index("tok"), lax.axis_index("col")
    z, y, core = tok // (WIDE * CORES), tok // CORES % WIDE, tok % CORES
    owner_z, owner_y, owner_core = owner // (WIDE * CORES), owner // CORES % WIDE, owner % CORES
    flip = owner_z >= DEPTH // 2
    owner_at = DEPTH - 1 - owner_z if flip else owner_z
    owner_position = owner_at * WIDE
    key_item = CHIPS + owner_position
    near_z = DEPTH - 1 - z if flip else z
    position = near_z * WIDE + (y + owner_y) % WIDE
    block, features = x_ref.shape
    piece = block // CUT
    head = slots_ref.shape[2]
    depth = slots_ref.shape[1]
    part = depth // CUT
    out_cols = cols_ref.shape[1]
    own_slot, key_slot = CHIPS, CHIPS + 1
    at_owner = position == owner_position
    is_owner = at_owner & (core == owner_core)
    is_fed = at_owner & (core != owner_core)

    def tok_at(where, which):
        at_z = where // WIDE
        at_z = DEPTH - 1 - at_z if flip else at_z
        return (at_z * WIDE + (where % WIDE + owner_y) % WIDE) * CORES + which

    up, down = (tok - WIDE * CORES, tok + WIDE * CORES) if flip else (tok + WIDE * CORES, tok - WIDE * CORES)
    beside = tok + CORES - 2 * CORES * y
    twin = tok + 1 - 2 * core
    partner = 1 - col
    neighbour = (beside, up, down)
    neighbour_position = (position + 1 - 2 * (position % WIDE), position + WIDE, position - WIDE)
    present = (y >= 0, near_z < DEPTH - 1, near_z > 0)

    barrier = pltpu.get_barrier_semaphore()
    for at, there in zip(neighbour, present):
        @pl.when(there)
        def _():
            pl.semaphore_signal(barrier, inc=1, device_id=(at, col), device_id_type=MESH)
    pl.semaphore_signal(barrier, inc=1, device_id=(twin, col), device_id_type=MESH)
    pl.semaphore_signal(barrier, inc=1, device_id=(tok, partner), device_id_type=MESH)
    pl.semaphore_signal(barrier, inc=1, device_id=(twin, partner), device_id_type=MESH)
    pl.semaphore_wait(barrier, 4 + jnp.minimum(near_z, 1) + jnp.minimum(DEPTH - 1 - near_z, 1))

    def remote(source, target, sent, received, at):
        return pltpu.make_async_remote_copy(
            src_ref=source, dst_ref=target, send_sem=sent, recv_sem=received, device_id=at, device_id_type=MESH
        )

    def rows_of(item, cut):
        return pl.ds(pl.multiple_of(tok_at(item, core) * block + cut * piece, piece), piece)

    def depth_of(cut):
        return pl.ds(pl.multiple_of(cut * part, part), part)

    def slot_of(item, at):
        where = item - CHIPS
        return jnp.where(item == key_item, key_slot + core, jnp.where(where == at, own_slot, where))

    gives_columns = z // (DEPTH // 2) == col

    def pass_tokens(item, cut):
        rows = rows_of(item, cut)
        remote(all_ref.at[rows], all_ref.at[rows], twin_send.at[0], twin_recv.at[0], (twin, col)).start()

        @pl.when(gives_columns)
        def _():
            for which in range(CORES):
                target = tok - core + which
                first = pl.multiple_of(target * out_cols % features, out_cols)
                remote(
                    all_ref.at[rows, pl.ds(first, out_cols)], cols_ref.at[rows],
                    cross_send.at[0], cross_recv.at[core], (target, partner),
                ).start()

    def pass_keys(cut):
        ref = slots_ref.at[key_slot + core, depth_of(cut)]
        remote(ref, ref, twin_send.at[1], twin_recv.at[1], (twin, col)).start()

    def pass_weights(cut):
        @pl.when(cut // (CUT // 2) == partner)
        def _():
            remote(
                slots_ref.at[own_slot, depth_of(cut)],
                other_ref.at[pl.ds(pl.multiple_of(cut % (CUT // 2) * part, part), part)],
                cross_send.at[1], cross_recv.at[2], (tok, partner),
            ).start()

    order = [owner_position]
    for step in range(len(step_entries(owner_at, 0, 0))):
        for direction in (1, 0, 2):
            entry = step_entries(owner_at, direction, owner_position)[step]
            item = (entry - 1) // CUT - CHIPS
            if entry and item >= 0 and item not in order:
                order.append(item)
    order = [item for item in order if item != owner_position] + [owner_position]

    def feed(item, cut):
        which = 1 - owner_core
        lane = tok_at(item, which) * head
        source = wq_ref.at[0, depth_of(cut), pl.ds(lane, head)]
        slot = own_slot if item == owner_position else item
        return remote(
            source, slots_ref.at[slot, depth_of(cut)], feed_sem.at[0, item, cut], feed_sem.at[1, item, cut], (twin, col)
        )

    def feed_keys(cut):
        which = 1 - owner_core
        return remote(
            wk_ref.at[0, depth_of(cut), pl.ds(which * head, head)], slots_ref.at[key_slot + which, depth_of(cut)],
            feed_sem.at[0, CHIPS, cut], feed_sem.at[1, CHIPS, cut], (twin, col),
        )

    @pl.when(is_owner)
    def _():
        for item in order[:2]:
            for cut in range(CUT):
                feed(item, cut).start()
        for cut in range(CUT):
            feed_keys(cut).start()
        for item in order[2:]:
            for cut in range(CUT):
                feed(item, cut).start()

    def own_rows():
        return pl.ds(pl.multiple_of(tok * block, block), block)

    take = pltpu.make_async_copy(x_ref, x_buf, local_sem.at[0])
    take.start()
    take.wait()
    put = pltpu.make_async_copy(x_buf, all_ref.at[own_rows()], local_sem.at[0])
    put.start()
    put.wait()

    @pl.when(is_owner)
    def _():
        for slot, source in (
            (key_slot + owner_core, wk_ref.at[0, :, pl.ds(owner_core * head, head)]),
            (own_slot, wq_ref.at[0, :, pl.ds(owner * head, head)]),
        ):
            take = pltpu.make_async_copy(source, w_buf, local_sem.at[1])
            take.start()
            take.wait()
            put = pltpu.make_async_copy(w_buf, slots_ref.at[slot], local_sem.at[1])
            put.start()
            put.wait()
        for cut in range(CUT):
            pass_keys(cut)
            pass_weights(cut)

    for cut in range(CUT):
        pass_tokens(position, cut)

    tables = [[packed_table(owner_at, direction, late) for direction in range(3)] for late in (False, True)]
    length = len(tables[0][0][0])
    mine = [
        [
            [choose(position, [tables[late][direction][p][i] for p in range(CHIPS)]) for i in range(length)]
            for direction in range(3)
        ]
        for late in range(2)
    ]

    def entry_at(late, direction, step):
        number = choose(step // PACK, mine[late][direction])
        shift = step % PACK
        return number // choose(shift, [BASE**j for j in range(PACK)]) % BASE

    def arrived(entry):
        item, cut = (entry - 1) // CUT, (entry - 1) % CUT
        rows = rows_of(0, 0)
        remote(all_ref.at[rows], all_ref.at[rows], send_sem.at[0, 0], recv_sem.at[entry - 1], (twin, col)).wait_recv()

        @pl.when(item < CHIPS)
        def _():
            pass_tokens(item, cut)

        @pl.when(item == key_item)
        def _():
            pass_keys(cut)

        @pl.when((item == position + CHIPS) & (item != key_item))
        def _():
            pass_weights(cut)

    def send_tokens(direction, entry, step):
        rows = rows_of((entry - 1) // CUT, (entry - 1) % CUT)
        return remote(
            all_ref.at[rows], all_ref.at[rows], send_sem.at[direction, step], recv_sem.at[entry - 1],
            (neighbour[direction], col),
        )

    def send_slot(direction, entry, step):
        item, cut = (entry - 1) // CUT, (entry - 1) % CUT
        return remote(
            slots_ref.at[slot_of(item, position), depth_of(cut)],
            slots_ref.at[slot_of(item, neighbour_position[direction]), depth_of(cut)],
            send_sem.at[direction, step], recv_sem.at[entry - 1], (neighbour[direction], col),
        )

    def send_stored(direction, entry, step):
        item, cut = (entry - 1) // CUT, (entry - 1) % CUT
        lane = pl.multiple_of(tok_at(item - CHIPS, core) * head, head)
        return remote(
            wq_ref.at[0, depth_of(cut), pl.ds(lane, head)],
            slots_ref.at[slot_of(item, neighbour_position[direction]), depth_of(cut)],
            send_sem.at[direction, step], recv_sem.at[entry - 1], (neighbour[direction], col),
        )

    def fed(entry):
        item, cut = (entry - 1) // CUT - CHIPS, (entry - 1) % CUT
        at = jnp.where(item == owner_position, CHIPS, item)
        ref = slots_ref.at[own_slot, depth_of(0)]
        remote(ref, ref, feed_sem.at[0, at, cut], feed_sem.at[1, at, cut], (twin, col)).wait_recv()

    key_step, head_step = 3, 8

    def step_body(step, carry):
        @pl.when(is_fed & (step == key_step))
        def _():
            for cut in range(CUT):
                feed_keys(cut).wait_recv()
                pass_keys(cut)

        @pl.when(is_fed & (step == head_step))
        def _():
            for cut in range(CUT):
                feed(owner_position, cut).wait_recv()
                pass_weights(cut)

        for direction in range(3):
            entry = entry_at(1, direction, step)

            @pl.when(entry > 0)
            def _():
                arrived(entry)

        for direction in range(3):
            entry = entry_at(0, direction, step)
            item = (entry - 1) // CUT
            stored = is_owner & (item != key_item)

            @pl.when((entry > 0) & (item < CHIPS))
            def _():
                send_tokens(direction, entry, step).start()

            @pl.when((item >= CHIPS) & is_fed & (item != key_item))
            def _():
                fed(entry)

            @pl.when((item >= CHIPS) & stored)
            def _():
                send_stored(direction, entry, step).start()

            @pl.when((item >= CHIPS) & jnp.logical_not(stored))
            def _():
                send_slot(direction, entry, step).start()

        return carry

    steps = length * PACK
    lax.fori_loop(0, steps, step_body, 0)

    def drain(step, carry):
        for direction in range(3):
            entry = entry_at(0, direction, step)

            @pl.when(entry > 0)
            def _():
                send_tokens(direction, jnp.int32(1), step).wait_send()

        return carry

    lax.fori_loop(0, steps, drain, 0)

    @pl.when(is_owner)
    def _():
        for item in order:
            for cut in range(CUT):
                feed(item, cut).wait_send()
        for cut in range(CUT):
            feed_keys(cut).wait_send()

    half = all_ref.shape[0] // CORES
    halves = all_ref.at[pl.ds(0, half)]
    remote(halves, halves, twin_send.at[0], twin_recv.at[0], (twin, col)).wait()
    keys = slots_ref.at[key_slot]
    remote(keys, keys, twin_send.at[1], twin_recv.at[1], (twin, col)).wait()
    remote(other_ref, other_ref, cross_send.at[1], cross_recv.at[2], (tok, partner)).wait()

    @pl.when(gives_columns)
    def _():
        remote(cols_ref, cols_ref, cross_send.at[0], cross_recv.at[0], (tok, partner)).wait_send()

    @pl.when(jnp.logical_not(gives_columns))
    def _():
        part_cols = cols_ref.at[pl.ds(0, half)]
        for which in range(CORES):
            remote(part_cols, part_cols, cross_send.at[0], cross_recv.at[which], (tok, partner)).wait_recv()


def exchange(owner, x_block, wq, wk):
    block, features = x_block.shape
    groups = CHIPS * CORES
    depth = wq.shape[1]
    head = wk.shape[2] // CORES
    out_cols = features * lax.axis_size("col") // groups
    steps = (len(step_entries(0, 0, 0)) + LAG + PACK - 1) // PACK * PACK
    kind = x_block.dtype
    any_space = pl.BlockSpec(memory_space=pl.ANY)
    return pl.pallas_call(
        functools.partial(exchange_kernel, owner),
        out_shape=(
            jax.ShapeDtypeStruct((groups * block, features), kind),
            jax.ShapeDtypeStruct((groups * block, out_cols), kind),
            jax.ShapeDtypeStruct((CHIPS + 3, depth, head), kind),
            jax.ShapeDtypeStruct((depth // 2, head), kind),
        ),
        in_specs=[any_space] * 3,
        out_specs=(any_space,) * 4,
        scratch_shapes=[
            pltpu.VMEM((block, features), kind),
            pltpu.VMEM((depth, head), kind),
            pltpu.SemaphoreType.DMA((2,)),
            pltpu.SemaphoreType.DMA((2 * CHIPS * CUT,)),
            pltpu.SemaphoreType.DMA((3, steps)),
            pltpu.SemaphoreType.DMA((2, CHIPS + 1, CUT)),
            pltpu.SemaphoreType.DMA((2,)),
            pltpu.SemaphoreType.DMA((2,)),
            pltpu.SemaphoreType.DMA((2,)),
            pltpu.SemaphoreType.DMA((3,)),
        ],
        compiler_params=pltpu.CompilerParams(collective_id=owner, has_side_effects=True),
    )(x_block, wq, wk)


def grid_shards(hidden, norm_gain, token_ids, owner, query_store, key_store):
    normed = normalize(hidden, norm_gain)
    place = positions(token_ids)
    tok, column = lax.axis_index("tok"), lax.axis_index("col")
    groups = lax.axis_size("tok")
    features = normed.shape[1] // lax.axis_size("col")
    x_block = lax.dynamic_slice_in_dim(normed, column * features, features, 1)
    total_tokens = normed.shape[0] * groups
    q_width, k_width = query_store.shape[2], key_store.shape[2]
    branches = [functools.partial(exchange, at) for at in range(groups)]
    gathered, sent_cols, slots, other = lax.switch(owner[0], branches, x_block, query_store, key_store)
    out_cols = sent_cols.shape[1]
    here = tok // (groups // 2) == column
    own_cols = lax.dynamic_slice_in_dim(gathered, tok * out_cols % features, out_cols, 1)
    col_block = jnp.where(here, own_cols, sent_cols)
    hessian = transposed_product(gathered, col_block) * (2.0 / total_tokens)
    own_weight = lax.dynamic_slice_in_dim(slots[CHIPS], column * features, features, 0)
    head = own_weight.shape[1]
    weight = jnp.concatenate([own_weight, other], axis=1)
    partial = jnp.dot(gathered, weight, preferred_element_type=jnp.float32).astype(jnp.bfloat16)
    crossed = lax.ppermute(partial[:, head:], "col", [(0, 1), (1, 0)])
    summed = (partial[:, :head].astype(jnp.float32) + crossed.astype(jnp.float32)).astype(jnp.bfloat16)
    raw_q = lax.all_to_all(summed, "tok", split_axis=0, concat_axis=1, tiled=True).astype(jnp.float32)
    weight_k = jnp.concatenate([slots[CHIPS + 1], slots[CHIPS + 2]], axis=1)
    raw_k = jnp.dot(normed, weight_k, preferred_element_type=jnp.float32)
    queries = rotate(raw_q, place, column * q_width).astype(jnp.bfloat16)
    keys = rotate(raw_k, place, column * k_width).astype(jnp.bfloat16)
    return (queries, keys, hessian)


def solution(mesh):
    placed = (P("tok", None), P(), P("tok"), P(), P("tok", None, "col"), P("tok", None, "col"))
    fits = mesh.shape["tok"] == CHIPS * CORES and mesh.shape["col"] == 2
    return jax.shard_map(
        grid_shards if fits else shards,
        mesh=mesh,
        in_specs=placed,
        out_specs=(P("tok", "col"), P("tok", "col"), P("col", "tok")),
        check_vma=False,
    )
```

```python
import functools

import jax
import jax.numpy as jnp
from jax import lax
from jax.experimental import pallas as pl
from jax.experimental.pallas import tpu as pltpu
from jax.sharding import PartitionSpec as P

HEAD = 128
SEQ = 128


begin_token = 128000
rope_base = 500000.0


def scatter_weights(query, key, owner):
    groups = lax.axis_size("tok")
    depth, width = query.shape
    piece = width // groups
    mine = lax.axis_index("tok") == owner
    query = jnp.moveaxis(query.reshape(depth, groups, piece), 1, 0)
    key = key.reshape(groups, depth * key.shape[1] // groups // piece, piece)
    both = jnp.concatenate([query, key], axis=1)
    return jnp.where(mine, both, jnp.zeros_like(both))


def positions(token_ids):
    samples = token_ids.reshape(-1, SEQ)
    index = jnp.arange(SEQ, dtype=jnp.int32)
    starts = jnp.where(samples == begin_token, index[None, :], jnp.zeros_like(samples))
    latest = lax.cummax(starts, axis=1)
    return (index[None, :] - latest).reshape(-1)


def rotate(values, place, start):
    width = values.shape[1]
    period = HEAD if width % HEAD == 0 else width
    dims = (start + jnp.arange(period, dtype=jnp.int32)) % HEAD
    pair = (dims // 2).astype(jnp.float32)
    freq = jnp.power(jnp.float32(rope_base), -2.0 * pair / HEAD)
    angle = place.astype(jnp.float32)[:, None] * freq[None, :]
    even = dims % 2 == 0
    sine = jnp.where(even[None, :], -jnp.sin(angle), jnp.sin(angle))
    cosine, sine = lax.optimization_barrier((jnp.cos(angle), sine))
    cosine = jnp.tile(cosine, (1, width // period))
    sine = jnp.tile(sine, (1, width // period))
    following = jnp.concatenate([values[:, 1:], values[:, :1]], axis=1)
    previous = jnp.concatenate([values[:, -1:], values[:, :-1]], axis=1)
    even = jnp.arange(width, dtype=jnp.int32) % 2 == 0
    other = jnp.where(even[None, :], following, previous)
    return values * cosine + other * sine


def normalize(hidden, norm_gain):
    wide = hidden.astype(jnp.float32)
    meansq = jnp.mean(wide * wide, axis=-1, keepdims=True)
    return (wide * lax.rsqrt(meansq + 1e-05) * norm_gain[None, :]).astype(jnp.bfloat16)


def transposed_product(left, right):
    return lax.dot_general(
        left, right, (((0,), (0,)), ((), ())), preferred_element_type=jnp.float32
    )


def shards(hidden, norm_gain, token_ids, owner, query_store, key_store):
    normed = normalize(hidden, norm_gain)
    place = positions(token_ids)
    column = lax.axis_index("col")
    row_width = normed.shape[1] // lax.axis_size("col")
    row_block = lax.dynamic_slice_in_dim(normed, column * row_width, row_width, 1)
    total_tokens = normed.shape[0] * lax.axis_size("tok")
    groups, parts = lax.axis_size("tok"), lax.axis_size("col")
    depth, q_width = query_store.shape[1:]
    k_width = key_store.shape[2]
    masked = scatter_weights(query_store[0], key_store[0], owner[0])
    gathered = lax.all_gather(row_block, "tok", axis=0, tiled=True)
    col_block = lax.all_to_all(normed, "tok", split_axis=1, concat_axis=0, tiled=True)
    masked, gathered = lax.optimization_barrier((masked, gathered))
    owned = lax.psum_scatter(masked, "tok", scatter_dimension=0, tiled=False)
    gram = transposed_product(gathered, col_block)
    hessian = gram * (2.0 / total_tokens)
    key_rows = owned[depth:].reshape(depth // groups, k_width)
    weight_k = lax.all_gather(key_rows, "tok", axis=0, tiled=True)
    weight_q = lax.all_to_all(owned[:depth], "col", split_axis=0, concat_axis=1, tiled=True)
    partial = jnp.dot(gathered, weight_q, preferred_element_type=jnp.float32).astype(jnp.bfloat16)
    partial = lax.all_to_all(partial, "col", split_axis=1, concat_axis=0, tiled=True)
    partial = partial.reshape(parts, total_tokens, q_width // groups).astype(jnp.float32)
    summed = jnp.sum(partial, axis=0).astype(jnp.bfloat16)
    raw_q = lax.all_to_all(summed, "tok", split_axis=0, concat_axis=1, tiled=True).astype(jnp.float32)
    raw_k = jnp.dot(normed, weight_k, preferred_element_type=jnp.float32)
    queries = rotate(raw_q, place, column * q_width).astype(jnp.bfloat16)
    keys = rotate(raw_k, place, column * k_width).astype(jnp.bfloat16)
    return (queries, keys, hessian)


MESH = pl.DeviceIdType.MESH

DEPTH, WIDE, CORES = 4, 2, 2
CHIPS = DEPTH * WIDE
CUT = 4
LAG = 2
BASE = 128
PACK = 4
ROUTES = (
    (
        (
            (8438017, 76075297, 135257917, 84529957, 59165977),
            (16892677, 46483213, 33803287, 0, 0),
            (25347337, 2321, 97208851, 6191, 0),
            (12664832, 8438017, 76075297, 46482439, 3095),
            (42256657, 25347337, 8438017, 114114560, 7223),
            (29575957, 50710543, 71844613, 16896547, 0),
            (59165977, 42256657, 4211977, 25346563, 0),
            (67620637, 29575957, 33800965, 3095, 1031),
        ),
        (
            (126803257, 118348597, 101439277, 109893937, 92984617),
            (4211461, 71844355, 16896547, 135257917, 0),
            (25347337, 4218169, 126796291, 118348597, 109893937),
            (33801997, 773, 76075297, 131023879, 8255),
            (42256657, 25347337, 8438017, 76075297, 126803257),
            (50711317, 12666637, 71845903, 16896547, 135257917),
            (0, 0, 0, 0, 0),
            (0, 0, 0, 0, 0),
        ),
        (
            (0, 0, 0, 0, 0),
            (0, 0, 0, 0, 0),
            (25347337, 59165977, 63392017, 42258463, 0),
            (33801997, 50711317, 25347337, 42256657, 67620637),
            (54937873, 42257947, 67620637, 33801997, 0),
            (50711317, 67620637, 59165977, 0, 0),
            (59165977, 67620637, 0, 0, 0),
            (67620637, 59165977, 0, 0, 0),
        ),
    ),
    (
        (
            (8438017, 42256657, 67620637, 50711317, 0),
            (29573120, 25347337, 59165977, 92984617, 2063),
            (25347337, 92984617, 84529957, 101439277, 0),
            (46483213, 12667927, 33801223, 0, 0),
            (42256657, 135257917, 8438017, 118348597, 0),
            (29575957, 21121039, 50710027, 88752128, 5675),
            (59165977, 29573120, 8438017, 21121039, 1547),
            (67620637, 50711317, 0, 16892677, 92984617),
        ),
        (
            (8438017, 0, 0, 0, 0),
            (16892677, 8438017, 0, 0, 0),
            (135257917, 8438017, 118348597, 126803257, 109893937),
            (33801997, 25347337, 16892677, 92984617, 0),
            (42256657, 4212493, 33800707, 25347337, 126803257),
            (50711317, 131025169, 12673087, 88753159, 42260011),
            (0, 0, 0, 0, 0),
            (0, 0, 0, 0, 0),
        ),
        (
            (0, 0, 0, 0, 0),
            (0, 0, 0, 0, 0),
            (38031649, 63392275, 46485535, 12667927, 76071943),
            (21120781, 54937099, 88755739, 33805867, 84529957),
            (42256657, 67620637, 59165977, 0, 0),
            (50711317, 59165977, 67620637, 42256657, 0),
            (63393049, 59166751, 0, 12664832, 1031),
            (54939421, 67620379, 0, 0, 0),
        ),
    ),
)


def step_entries(owner_at, direction, position):
    entries = []
    for number in ROUTES[owner_at][direction][position]:
        for _ in range(PACK):
            entries.append(number % BASE)
            number //= BASE
    return entries


def packed_table(owner_at, direction, arrivals):
    table = []
    for position in range(CHIPS):
        entries = None
        if not arrivals:
            entries = step_entries(owner_at, direction, position) + [0] * LAG
        else:
            z = position // WIDE + (0, -1, 1)[direction]
            sender = position ^ 1 if direction == 0 else z * WIDE + position % WIDE
            entries = [0] * LAG + (
                step_entries(owner_at, direction, sender) if 0 <= z < DEPTH else [0] * len(step_entries(owner_at, 0, 0))
            )
        entries += [0] * (-len(entries) % PACK)
        table.append([
            sum(entries[i + j] * BASE**j for j in range(PACK)) for i in range(0, len(entries), PACK)
        ])
    return table


def choose(index, options):
    value = jnp.int32(0)
    for at, option in enumerate(options):
        if isinstance(option, int) and option == 0:
            continue
        value = jnp.where(index == at, jnp.int32(option) if isinstance(option, int) else option, value)
    return value


def exchange_kernel(
    owner, x_ref, wq_ref, wk_ref, all_ref, cols_ref, slots_ref, other_ref,
    x_buf, w_buf, local_sem, recv_sem, send_sem, feed_sem, twin_send, twin_recv, cross_send, cross_recv,
):
    tok, col = lax.axis_index("tok"), lax.axis_index("col")
    z, y, core = tok // (WIDE * CORES), tok // CORES % WIDE, tok % CORES
    owner_z, owner_y, owner_core = owner // (WIDE * CORES), owner // CORES % WIDE, owner % CORES
    flip = owner_z >= DEPTH // 2
    owner_at = DEPTH - 1 - owner_z if flip else owner_z
    owner_position = owner_at * WIDE
    key_item = CHIPS + owner_position
    near_z = DEPTH - 1 - z if flip else z
    position = near_z * WIDE + (y + owner_y) % WIDE
    block, features = x_ref.shape
    piece = block // CUT
    head = slots_ref.shape[2]
    depth = slots_ref.shape[1]
    part = depth // CUT
    out_cols = cols_ref.shape[1]
    own_slot, key_slot = CHIPS, CHIPS + 1
    at_owner = position == owner_position
    is_owner = at_owner & (core == owner_core)
    is_fed = at_owner & (core != owner_core)

    def tok_at(where, which):
        at_z = where // WIDE
        at_z = DEPTH - 1 - at_z if flip else at_z
        return (at_z * WIDE + (where % WIDE + owner_y) % WIDE) * CORES + which

    up, down = (tok - WIDE * CORES, tok + WIDE * CORES) if flip else (tok + WIDE * CORES, tok - WIDE * CORES)
    beside = tok + CORES - 2 * CORES * y
    twin = tok + 1 - 2 * core
    partner = 1 - col
    neighbour = (beside, up, down)
    neighbour_position = (position + 1 - 2 * (position % WIDE), position + WIDE, position - WIDE)
    present = (y >= 0, near_z < DEPTH - 1, near_z > 0)

    barrier = pltpu.get_barrier_semaphore()
    for at, there in zip(neighbour, present):
        @pl.when(there)
        def _():
            pl.semaphore_signal(barrier, inc=1, device_id=(at, col), device_id_type=MESH)
    pl.semaphore_signal(barrier, inc=1, device_id=(twin, col), device_id_type=MESH)
    pl.semaphore_signal(barrier, inc=1, device_id=(tok, partner), device_id_type=MESH)
    pl.semaphore_signal(barrier, inc=1, device_id=(twin, partner), device_id_type=MESH)
    pl.semaphore_wait(barrier, 4 + jnp.minimum(near_z, 1) + jnp.minimum(DEPTH - 1 - near_z, 1))

    def remote(source, target, sent, received, at):
        return pltpu.make_async_remote_copy(
            src_ref=source, dst_ref=target, send_sem=sent, recv_sem=received, device_id=at, device_id_type=MESH
        )

    def rows_of(item, cut):
        return pl.ds(pl.multiple_of(tok_at(item, core) * block + cut * piece, piece), piece)

    def depth_of(cut):
        return pl.ds(pl.multiple_of(cut * part, part), part)

    def slot_of(item, at):
        where = item - CHIPS
        return jnp.where(item == key_item, key_slot + core, jnp.where(where == at, own_slot, where))

    gives_columns = z // (DEPTH // 2) == col

    def loop(count, body):
        def step(at, carry):
            body(at)
            return carry

        lax.fori_loop(0, count, step, 0)

    def columns_of(target):
        return pl.ds(pl.multiple_of(target * out_cols % features, out_cols), out_cols)

    def keep_columns(rows):
        return pltpu.make_async_copy(all_ref.at[rows, columns_of(tok)], cols_ref.at[rows], local_sem.at[2])

    def pass_tokens(item, cut):
        rows = rows_of(item, cut)
        remote(all_ref.at[rows], all_ref.at[rows], twin_send.at[0], twin_recv.at[0], (twin, col)).start()

        @pl.when(gives_columns)
        def _():
            keep_columns(rows).start()

            def give(at):
                target = jnp.where(at == 0, twin, tok - core + at - 1)
                plane = jnp.where(at == 0, col, partner)
                remote(
                    all_ref.at[rows, columns_of(target)], cols_ref.at[rows], cross_send.at[0], cross_recv.at[core],
                    (target, plane),
                ).start()

            loop(1 + CORES, give)

    def pass_keys(cut):
        ref = slots_ref.at[key_slot + core, depth_of(cut)]
        remote(ref, ref, twin_send.at[1], twin_recv.at[1], (twin, col)).start()

    def pass_weights(cut):
        @pl.when(cut // (CUT // 2) == partner)
        def _():
            remote(
                slots_ref.at[own_slot, depth_of(cut)],
                other_ref.at[pl.ds(pl.multiple_of(cut % (CUT // 2) * part, part), part)],
                cross_send.at[1], cross_recv.at[2], (tok, partner),
            ).start()

    order = []
    for step in range(len(step_entries(owner_at, 0, 0))):
        for direction in (1, 0, 2):
            entry = step_entries(owner_at, direction, owner_position)[step]
            item = (entry - 1) // CUT - CHIPS
            if entry and item >= 0 and item not in order and item != owner_position:
                order.append(item)
    order.append(owner_position)
    fed_core = 1 - owner_core

    def feed(item, cut):
        lane = pl.multiple_of(tok_at(item, fed_core) * head, head)
        slot = jnp.where(item == owner_position, own_slot, item)
        return remote(
            wq_ref.at[0, depth_of(cut), pl.ds(lane, head)], slots_ref.at[slot, depth_of(cut)],
            feed_sem.at[0, item * CUT + cut], feed_sem.at[1, item * CUT + cut], (twin, col),
        )

    def feed_keys(cut):
        return remote(
            wk_ref.at[0, depth_of(cut), pl.ds(fed_core * head, head)],
            slots_ref.at[key_slot + fed_core, depth_of(cut)],
            feed_sem.at[0, CHIPS * CUT + cut], feed_sem.at[1, CHIPS * CUT + cut], (twin, col),
        )

    def feed_some(first, last):
        loop((last - first) * CUT, lambda at: feed(choose(at // CUT + first, order), at % CUT).start())

    @pl.when(is_owner)
    def _():
        feed_some(0, 2)
        loop(CUT, lambda cut: feed_keys(cut).start())
        feed_some(2, CHIPS)

    def through(source, buffer, target, sem):
        take = pltpu.make_async_copy(source, buffer, sem)
        take.start()
        take.wait()
        put = pltpu.make_async_copy(buffer, target, sem)
        put.start()
        put.wait()

    through(x_ref, x_buf, all_ref.at[pl.ds(pl.multiple_of(tok * block, block), block)], local_sem.at[0])

    @pl.when(is_owner)
    def _():
        through(
            wk_ref.at[0, :, pl.ds(owner_core * head, head)], w_buf, slots_ref.at[key_slot + owner_core], local_sem.at[1]
        )
        through(wq_ref.at[0, :, pl.ds(owner * head, head)], w_buf, slots_ref.at[own_slot], local_sem.at[1])
        loop(CUT, pass_keys)
        loop(CUT, pass_weights)

    loop(CUT, lambda cut: pass_tokens(position, cut))

    tables = [[packed_table(owner_at, direction, late) for direction in range(3)] for late in (False, True)]
    length = len(tables[0][0][0])
    mine = [
        [
            choose(position, [tables[late][direction][p][i] for p in range(CHIPS)])
            for direction in range(3)
            for i in range(length)
        ]
        for late in range(2)
    ]

    def entry_at(late, direction, step):
        number = choose(direction * length + step // PACK, mine[late])
        return number // choose(step % PACK, [BASE**j for j in range(PACK)]) % BASE

    def arrived(entry):
        item, cut = (entry - 1) // CUT, (entry - 1) % CUT
        rows = rows_of(0, 0)
        remote(all_ref.at[rows], all_ref.at[rows], send_sem.at[0, 0], recv_sem.at[entry - 1], (twin, col)).wait_recv()

        @pl.when(item < CHIPS)
        def _():
            pass_tokens(item, cut)

        @pl.when(item == key_item)
        def _():
            pass_keys(cut)

        @pl.when((item == position + CHIPS) & (item != key_item))
        def _():
            pass_weights(cut)

    def send(source, target, direction, entry, step):
        return remote(
            source, target, send_sem.at[direction, step], recv_sem.at[entry - 1], (choose(direction, neighbour), col)
        )

    def send_tokens(direction, entry, step):
        rows = rows_of((entry - 1) // CUT, (entry - 1) % CUT)
        return send(all_ref.at[rows], all_ref.at[rows], direction, entry, step)

    def send_weights(direction, entry, step, stored):
        item, cut = (entry - 1) // CUT, (entry - 1) % CUT
        target = slots_ref.at[slot_of(item, choose(direction, neighbour_position)), depth_of(cut)]
        lane = pl.multiple_of(tok_at(item - CHIPS, core) * head, head)
        if stored:
            source = wq_ref.at[0, depth_of(cut), pl.ds(lane, head)]
        else:
            source = slots_ref.at[slot_of(item, position), depth_of(cut)]
        return send(source, target, direction, entry, step)

    def fed(at):
        ref = slots_ref.at[own_slot, depth_of(0)]
        remote(ref, ref, feed_sem.at[0, at], feed_sem.at[1, at], (twin, col)).wait_recv()

    key_step, head_step = 3, 8

    def step_body(step):
        @pl.when(is_fed & (step == key_step))
        def _():
            def take(cut):
                fed(CHIPS * CUT + cut)
                pass_keys(cut)

            loop(CUT, take)

        @pl.when(is_fed & (step == head_step))
        def _():
            def take(cut):
                fed(owner_position * CUT + cut)
                pass_weights(cut)

            loop(CUT, take)

        def receive(direction):
            entry = entry_at(1, direction, step)

            @pl.when(entry > 0)
            def _():
                arrived(entry)

        loop(3, receive)

        def forward(direction):
            entry = entry_at(0, direction, step)
            item = (entry - 1) // CUT
            stored = is_owner & (item != key_item)

            @pl.when((entry > 0) & (item < CHIPS))
            def _():
                send_tokens(direction, entry, step).start()

            @pl.when((item >= CHIPS) & is_fed & (item != key_item))
            def _():
                fed(entry - 1 - CHIPS * CUT)

            @pl.when((item >= CHIPS) & stored)
            def _():
                send_weights(direction, entry, step, True).start()

            @pl.when((item >= CHIPS) & jnp.logical_not(stored))
            def _():
                send_weights(direction, entry, step, False).start()

        loop(3, forward)

    steps = length * PACK
    loop(steps, step_body)

    def drain(at):
        step, direction = at // 3, at % 3

        @pl.when(entry_at(0, direction, step) > 0)
        def _():
            send_tokens(direction, jnp.int32(1), step).wait_send()

    loop(3 * steps, drain)

    @pl.when(is_owner)
    def _():
        loop(CHIPS * CUT, lambda at: feed(at // CUT, at % CUT).wait_send())
        loop(CUT, lambda cut: feed_keys(cut).wait_send())

    half = all_ref.shape[0] // CORES
    halves = all_ref.at[pl.ds(0, half)]
    remote(halves, halves, twin_send.at[0], twin_recv.at[0], (twin, col)).wait()
    keys = slots_ref.at[key_slot]
    remote(keys, keys, twin_send.at[1], twin_recv.at[1], (twin, col)).wait()
    remote(other_ref, other_ref, cross_send.at[1], cross_recv.at[2], (tok, partner)).wait()
    part_cols = cols_ref.at[pl.ds(0, half)]
    remote(part_cols, part_cols, cross_send.at[0], cross_recv.at[1 - core], (tok, partner)).wait_recv()

    @pl.when(gives_columns)
    def _():
        pltpu.make_async_copy(part_cols, part_cols, local_sem.at[2]).wait()
        given = all_ref.at[pl.ds(0, (1 + CORES) * half * out_cols // features)]
        remote(given, given, cross_send.at[0], cross_recv.at[0], (tok, partner)).wait_send()

    @pl.when(jnp.logical_not(gives_columns))
    def _():
        remote(part_cols, part_cols, cross_send.at[0], cross_recv.at[core], (tok, partner)).wait_recv()


def exchange(owner, x_block, wq, wk):
    block, features = x_block.shape
    groups = CHIPS * CORES
    depth = wq.shape[1]
    head = wk.shape[2] // CORES
    out_cols = features * lax.axis_size("col") // groups
    steps = (len(step_entries(0, 0, 0)) + LAG + PACK - 1) // PACK * PACK
    kind = x_block.dtype
    any_space = pl.BlockSpec(memory_space=pl.ANY)
    return pl.pallas_call(
        functools.partial(exchange_kernel, owner),
        out_shape=(
            jax.ShapeDtypeStruct((groups * block, features), kind),
            jax.ShapeDtypeStruct((groups * block, out_cols), kind),
            jax.ShapeDtypeStruct((CHIPS + 3, depth, head), kind),
            jax.ShapeDtypeStruct((depth // 2, head), kind),
        ),
        in_specs=[any_space] * 3,
        out_specs=(any_space,) * 4,
        scratch_shapes=[
            pltpu.VMEM((block, features), kind),
            pltpu.VMEM((depth, head), kind),
            pltpu.SemaphoreType.DMA((3,)),
            pltpu.SemaphoreType.DMA((2 * CHIPS * CUT,)),
            pltpu.SemaphoreType.DMA((3, steps)),
            pltpu.SemaphoreType.DMA((2, (CHIPS + 1) * CUT)),
            pltpu.SemaphoreType.DMA((2,)),
            pltpu.SemaphoreType.DMA((2,)),
            pltpu.SemaphoreType.DMA((2,)),
            pltpu.SemaphoreType.DMA((3,)),
        ],
        compiler_params=pltpu.CompilerParams(collective_id=owner, has_side_effects=True),
    )(x_block, wq, wk)


def finish_kernel(
    all_ref, slots_ref, other_ref, cos_ref, sin_ref, out_ref,
    w_buf, g_buf, own_buf, part_buf, part_recv, sum_buf, heads, load_sem, w_sem, part_sem, sum_sem, head_sem, keep_sem,
):
    tok, col = lax.axis_index("tok"), lax.axis_index("col")
    groups = CHIPS * CORES
    chip, partner = tok // CORES, 1 - col
    features, head = other_ref.shape
    rows = all_ref.shape[0] // CHIPS
    block = rows // CORES

    barrier = pltpu.get_barrier_semaphore()

    def greet(at, carry):
        pl.semaphore_signal(barrier, inc=1, device_id=(lax.rem(tok + at, groups), col), device_id_type=MESH)
        return carry

    lax.fori_loop(1, groups, greet, 0)
    pl.semaphore_signal(barrier, inc=1, device_id=(tok, partner), device_id_type=MESH)

    def load(at):
        where = lax.rem(chip + 1 + at, CHIPS)
        return pltpu.make_async_copy(
            all_ref.at[pl.ds(pl.multiple_of(where * rows, rows), rows)], g_buf.at[at % 2], load_sem.at[at % 2]
        )

    load(0).start()
    own = pltpu.make_async_copy(
        slots_ref.at[CHIPS, pl.ds(pl.multiple_of(col * features, features), features)],
        w_buf.at[:, pl.ds(0, head)], w_sem.at[0],
    )
    own.start()
    crossed = pltpu.make_async_copy(other_ref, w_buf.at[:, pl.ds(head, head)], w_sem.at[1])
    crossed.start()
    own.wait()
    crossed.wait()
    pl.semaphore_wait(barrier, groups)

    def cross(at):
        return pltpu.make_async_remote_copy(
            src_ref=part_buf.at[at], dst_ref=part_recv.at[at], send_sem=part_sem.at[0, at], recv_sem=part_sem.at[1, at],
            device_id=(tok, partner), device_id_type=MESH,
        )

    def hand(at, which):
        source = sum_buf.at[at, pl.ds(which * block, block)]
        target = lax.rem(chip + 1 + at, CHIPS) * CORES + which
        return target, source, pltpu.make_async_remote_copy(
            src_ref=source, dst_ref=heads.at[tok], send_sem=sum_sem.at[at, which], recv_sem=head_sem.at[0],
            device_id=(target, col), device_id_type=MESH,
        )

    def body(at, carry):
        @pl.when(at < CHIPS)
        def _():
            load(at).wait()

        @pl.when(at + 1 < CHIPS)
        def _():
            load(at + 1).start()

        @pl.when((at >= 1) & (at < CHIPS + 1))
        def _():
            cross(at - 1).start()

        @pl.when(at >= 3)
        def _():
            for which in range(CORES):
                target, source, copy = hand(at - 3, which)

                @pl.when(target != tok)
                def _():
                    copy.start()

                @pl.when(target == tok)
                def _():
                    pltpu.make_async_copy(source, heads.at[tok], keep_sem.at[0]).start()

        @pl.when(at < CHIPS)
        def _():
            part = jnp.dot(g_buf[at % 2], w_buf[...], preferred_element_type=jnp.float32)
            own_buf[at] = part[:, :head]
            part_buf[at] = part[:, head:].astype(part_buf.dtype)

        @pl.when((at >= 2) & (at < CHIPS + 2))
        def _():
            cross(at - 2).wait_recv()
            sum_buf[at - 2] = (own_buf[at - 2] + part_recv[at - 2].astype(jnp.float32)).astype(sum_buf.dtype)

        return carry

    lax.fori_loop(0, CHIPS + 3, body, 0)

    def drain(at, carry):
        cross(at).wait_send()
        for which in range(CORES):
            target, source, copy = hand(at, which)

            @pl.when(target != tok)
            def _():
                copy.wait_send()

            @pl.when(target == tok)
            def _():
                pltpu.make_async_copy(source, heads.at[tok], keep_sem.at[0]).wait()

        return carry

    lax.fori_loop(0, CHIPS, drain, 0)
    others = heads.at[pl.ds(0, groups - 1)]
    pltpu.make_async_remote_copy(
        src_ref=others, dst_ref=others, send_sem=sum_sem.at[0, 0], recv_sem=head_sem.at[0],
        device_id=(tok, partner), device_id_type=MESH,
    ).wait_recv()

    even = lax.broadcasted_iota(jnp.int32, (block, head), 1) % 2 == 0
    for at in range(groups):
        raw = heads[at].astype(jnp.float32)
        swapped = jnp.where(even, pltpu.roll(raw, head - 1, 1), pltpu.roll(raw, 1, 1))
        out_ref[:, at * head : (at + 1) * head] = (raw * cos_ref[...] + swapped * sin_ref[...]).astype(out_ref.dtype)


def finish(gathered, slots, other, cosine, sine):
    features, head = other.shape
    groups = CHIPS * CORES
    rows = gathered.shape[0] // CHIPS
    block = rows // CORES
    kind = gathered.dtype
    any_space = pl.BlockSpec(memory_space=pl.ANY)
    vmem = pl.BlockSpec(memory_space=pltpu.VMEM)
    return pl.pallas_call(
        finish_kernel,
        out_shape=jax.ShapeDtypeStruct((block, groups * head), kind),
        in_specs=[any_space] * 3 + [vmem] * 2,
        out_specs=vmem,
        scratch_shapes=[
            pltpu.VMEM((features, 2 * head), kind),
            pltpu.VMEM((2, rows, features), kind),
            pltpu.VMEM((CHIPS, rows, head), jnp.float32),
            pltpu.VMEM((CHIPS, rows, head), kind),
            pltpu.VMEM((CHIPS, rows, head), kind),
            pltpu.VMEM((CHIPS, rows, head), kind),
            pltpu.VMEM((groups, block, head), kind),
            pltpu.SemaphoreType.DMA((2,)),
            pltpu.SemaphoreType.DMA((2,)),
            pltpu.SemaphoreType.DMA((2, CHIPS)),
            pltpu.SemaphoreType.DMA((CHIPS, CORES)),
            pltpu.SemaphoreType.DMA((1,)),
            pltpu.SemaphoreType.DMA((1,)),
        ],
        compiler_params=pltpu.CompilerParams(collective_id=groups, has_side_effects=True),
    )(gathered, slots, other, cosine, sine)


def angles(place):
    dims = jnp.arange(HEAD, dtype=jnp.int32)
    pair = (dims // 2).astype(jnp.float32)
    freq = jnp.power(jnp.float32(rope_base), -2.0 * pair / HEAD)
    angle = place.astype(jnp.float32)[:, None] * freq[None, :]
    sine = jnp.where((dims % 2 == 0)[None, :], -jnp.sin(angle), jnp.sin(angle))
    return jnp.cos(angle), sine


def turn(values, cosine, sine):
    heads = values.shape[1] // HEAD
    even = jnp.arange(values.shape[1], dtype=jnp.int32) % 2 == 0
    other = jnp.where(even[None, :], jnp.roll(values, -1, axis=1), jnp.roll(values, 1, axis=1))
    return values * jnp.tile(cosine, (1, heads)) + other * jnp.tile(sine, (1, heads))


def grid_shards(hidden, norm_gain, token_ids, owner, query_store, key_store):
    normed = normalize(hidden, norm_gain)
    cosine, sine = lax.optimization_barrier(angles(positions(token_ids)))
    column = lax.axis_index("col")
    groups = lax.axis_size("tok")
    features = normed.shape[1] // lax.axis_size("col")
    x_block = lax.dynamic_slice_in_dim(normed, column * features, features, 1)
    total_tokens = normed.shape[0] * groups
    branches = [functools.partial(exchange, at) for at in range(groups)]
    gathered, col_block, slots, other = lax.switch(owner[0], branches, x_block, query_store, key_store)
    queries = finish(gathered, slots, other, cosine, sine)
    hessian = transposed_product(gathered, col_block) * (2.0 / total_tokens)
    weight_k = jnp.concatenate([slots[CHIPS + 1], slots[CHIPS + 2]], axis=1)
    raw_k = jnp.dot(normed, weight_k, preferred_element_type=jnp.float32)
    keys = turn(raw_k, cosine, sine).astype(jnp.bfloat16)
    return (queries, keys, hessian)


def solution(mesh):
    placed = (P("tok", None), P(), P("tok"), P(), P("tok", None, "col"), P("tok", None, "col"))
    fits = mesh.shape["tok"] == CHIPS * CORES and mesh.shape["col"] == 2
    return jax.shard_map(
        grid_shards if fits else shards,
        mesh=mesh,
        in_specs=placed,
        out_specs=(P("tok", "col"), P("tok", "col"), P("col", "tok")),
        check_vma=False,
    )
```

```python
import functools

import jax
import jax.numpy as jnp
from jax import lax
from jax.experimental import pallas as pl
from jax.experimental.pallas import tpu as pltpu
from jax.sharding import PartitionSpec as P

HEAD = 128
SEQ = 128


begin_token = 128000
rope_base = 500000.0


def scatter_weights(query, key, owner):
    groups = lax.axis_size("tok")
    depth, width = query.shape
    piece = width // groups
    mine = lax.axis_index("tok") == owner
    query = jnp.moveaxis(query.reshape(depth, groups, piece), 1, 0)
    key = key.reshape(groups, depth * key.shape[1] // groups // piece, piece)
    both = jnp.concatenate([query, key], axis=1)
    return jnp.where(mine, both, jnp.zeros_like(both))


def positions(token_ids):
    samples = token_ids.reshape(-1, SEQ)
    index = jnp.arange(SEQ, dtype=jnp.int32)
    starts = jnp.where(samples == begin_token, index[None, :], jnp.zeros_like(samples))
    latest = lax.cummax(starts, axis=1)
    return (index[None, :] - latest).reshape(-1)


def rotate(values, place, start):
    width = values.shape[1]
    period = HEAD if width % HEAD == 0 else width
    dims = (start + jnp.arange(period, dtype=jnp.int32)) % HEAD
    pair = (dims // 2).astype(jnp.float32)
    freq = jnp.power(jnp.float32(rope_base), -2.0 * pair / HEAD)
    angle = place.astype(jnp.float32)[:, None] * freq[None, :]
    even = dims % 2 == 0
    sine = jnp.where(even[None, :], -jnp.sin(angle), jnp.sin(angle))
    cosine, sine = lax.optimization_barrier((jnp.cos(angle), sine))
    cosine = jnp.tile(cosine, (1, width // period))
    sine = jnp.tile(sine, (1, width // period))
    following = jnp.concatenate([values[:, 1:], values[:, :1]], axis=1)
    previous = jnp.concatenate([values[:, -1:], values[:, :-1]], axis=1)
    even = jnp.arange(width, dtype=jnp.int32) % 2 == 0
    other = jnp.where(even[None, :], following, previous)
    return values * cosine + other * sine


def normalize(hidden, norm_gain):
    wide = hidden.astype(jnp.float32)
    meansq = jnp.mean(wide * wide, axis=-1, keepdims=True)
    return (wide * lax.rsqrt(meansq + 1e-05) * norm_gain[None, :]).astype(jnp.bfloat16)


def transposed_product(left, right):
    return lax.dot_general(
        left, right, (((0,), (0,)), ((), ())), preferred_element_type=jnp.float32
    )


def shards(hidden, norm_gain, token_ids, owner, query_store, key_store):
    normed = normalize(hidden, norm_gain)
    place = positions(token_ids)
    column = lax.axis_index("col")
    row_width = normed.shape[1] // lax.axis_size("col")
    row_block = lax.dynamic_slice_in_dim(normed, column * row_width, row_width, 1)
    total_tokens = normed.shape[0] * lax.axis_size("tok")
    groups, parts = lax.axis_size("tok"), lax.axis_size("col")
    depth, q_width = query_store.shape[1:]
    k_width = key_store.shape[2]
    masked = scatter_weights(query_store[0], key_store[0], owner[0])
    gathered = lax.all_gather(row_block, "tok", axis=0, tiled=True)
    col_block = lax.all_to_all(normed, "tok", split_axis=1, concat_axis=0, tiled=True)
    masked, gathered = lax.optimization_barrier((masked, gathered))
    owned = lax.psum_scatter(masked, "tok", scatter_dimension=0, tiled=False)
    gram = transposed_product(gathered, col_block)
    hessian = gram * (2.0 / total_tokens)
    key_rows = owned[depth:].reshape(depth // groups, k_width)
    weight_k = lax.all_gather(key_rows, "tok", axis=0, tiled=True)
    weight_q = lax.all_to_all(owned[:depth], "col", split_axis=0, concat_axis=1, tiled=True)
    partial = jnp.dot(gathered, weight_q, preferred_element_type=jnp.float32).astype(jnp.bfloat16)
    partial = lax.all_to_all(partial, "col", split_axis=1, concat_axis=0, tiled=True)
    partial = partial.reshape(parts, total_tokens, q_width // groups).astype(jnp.float32)
    summed = jnp.sum(partial, axis=0).astype(jnp.bfloat16)
    raw_q = lax.all_to_all(summed, "tok", split_axis=0, concat_axis=1, tiled=True).astype(jnp.float32)
    raw_k = jnp.dot(normed, weight_k, preferred_element_type=jnp.float32)
    queries = rotate(raw_q, place, column * q_width).astype(jnp.bfloat16)
    keys = rotate(raw_k, place, column * k_width).astype(jnp.bfloat16)
    return (queries, keys, hessian)


MESH = pl.DeviceIdType.MESH

DEPTH, WIDE, CORES = 4, 2, 2
CHIPS = DEPTH * WIDE
CUT = 4
LAG = 2
BASE = 128
PACK = 4
ROUTES = (
    (
        (
            (76078909, 8438017, 114118945, 80303143, 25347337),
            (29573893, 42255367, 4127, 0, 0),
            (38028553, 25349401, 97213495, 6191, 0),
            (29575183, 76071685, 8438017, 16896031, 0),
            (38029843, 25354303, 76074265, 8438017, 0),
            (29575957, 21122071, 33800965, 71843840, 1031),
            (38030875, 29575957, 3353, 4215331, 25346563),
            (67620637, 21121555, 3095, 33800965, 16896289),
        ),
        (
            (126804031, 118349113, 101439277, 109893937, 88757803),
            (131023621, 4215331, 71844355, 114115591, 0),
            (135251467, 122576443, 4215331, 105660931, 6707),
            (21120781, 12672829, 118343695, 16896289, 6965),
            (46483729, 126797581, 76078393, 8438017, 1547),
            (42257431, 135251209, 12672829, 71845903, 1031),
            (0, 0, 0, 0, 0),
            (0, 0, 0, 0, 0),
        ),
        (
            (0, 0, 0, 0, 0),
            (0, 0, 0, 0, 0),
            (25347337, 46483729, 63393307, 33803287, 3353),
            (46483213, 67619347, 63393307, 38030359, 54937615),
            (54937873, 59165461, 50712349, 2579, 4385),
            (42257173, 59166751, 50712349, 0, 0),
            (59165977, 67620637, 0, 0, 0),
            (59166751, 3869, 0, 0, 0),
        ),
    ),
    (
        (
            (88752385, 8443435, 21121555, 25349143, 3353),
            (29573893, 46483471, 63393307, 16894225, 4127),
            (84533053, 118346533, 101439277, 25347337, 0),
            (50710285, 16893967, 12668701, 4127, 0),
            (135252241, 42254851, 21122329, 114116107, 0),
            (29575957, 4211719, 92982295, 33800965, 0),
            (42257947, 29575441, 4211977, 54937099, 1031),
            (67620637, 50711317, 88752643, 12670507, 2063),
        ),
        (
            (4211203, 0, 0, 0, 0),
            (4211719, 92984617, 8438533, 0, 0),
            (8446015, 25347337, 122576443, 105667381, 6707),
            (16893709, 88752385, 12670507, 131024911, 7223),
            (38029843, 21120781, 25346305, 126796807, 7481),
            (50711317, 8446015, 92984617, 33800965, 7997),
            (0, 0, 0, 0, 0),
            (0, 0, 0, 0, 0),
        ),
        (
            (0, 0, 0, 0, 0),
            (0, 0, 0, 0, 0),
            (92984617, 21121555, 25349143, 76074265, 4385),
            (33801997, 59165461, 38031133, 84529183, 4901),
            (54938131, 59165461, 2321, 0, 0),
            (46484503, 63393307, 67619089, 54938131, 0),
            (59165977, 67620637, 0, 5417, 0),
            (59166493, 4127, 0, 0, 0),
        ),
    ),
)


def step_entries(owner_at, direction, position):
    entries = []
    for number in ROUTES[owner_at][direction][position]:
        for _ in range(PACK):
            entries.append(number % BASE)
            number //= BASE
    return entries


def packed_table(owner_at, direction, arrivals):
    table = []
    for position in range(CHIPS):
        entries = None
        if not arrivals:
            entries = step_entries(owner_at, direction, position) + [0] * LAG
        else:
            z = position // WIDE + (0, -1, 1)[direction]
            sender = position ^ 1 if direction == 0 else z * WIDE + position % WIDE
            entries = [0] * LAG + (
                step_entries(owner_at, direction, sender) if 0 <= z < DEPTH else [0] * len(step_entries(owner_at, 0, 0))
            )
        entries += [0] * (-len(entries) % PACK)
        table.append([
            sum(entries[i + j] * BASE**j for j in range(PACK)) for i in range(0, len(entries), PACK)
        ])
    return table


def choose(index, options):
    value = jnp.int32(0)
    for at, option in enumerate(options):
        if isinstance(option, int) and option == 0:
            continue
        value = jnp.where(index == at, jnp.int32(option) if isinstance(option, int) else option, value)
    return value


def arrival_steps(owner_at):
    steps = [[None] * (2 * CHIPS) for _ in range(CHIPS)]
    for position in range(CHIPS):
        for direction in range(3):
            z = position // WIDE + (0, 1, -1)[direction]
            target = position ^ 1 if direction == 0 else z * WIDE + position % WIDE
            for step, entry in enumerate(step_entries(owner_at, direction, position)):
                if entry:
                    item = (entry - 1) // CUT
                    steps[target][item] = max(steps[target][item] or 0, step + LAG)
    return steps


SLOTS = 2


def send_steps(owner_at):
    return (len(step_entries(owner_at, 0, 0)) + LAG + PACK - 1) // PACK * PACK


def job_table(owner_at):
    table = []
    for position, steps in enumerate(arrival_steps(owner_at)):
        ready = [1 if item == position else steps[item] + 1 for item in range(CHIPS)]
        waiting = sorted(range(CHIPS), key=lambda item: (ready[item], item))
        jobs = []
        while waiting:
            step = len(jobs) // SLOTS
            jobs.append(waiting.pop(0) + 1 if ready[waiting[0]] <= step else 0)
        table.append(jobs)
    slots = max(len(jobs) for jobs in table)
    packed = []
    for jobs in table:
        jobs = jobs + [0] * (-slots % PACK + slots - len(jobs))
        packed.append([sum(jobs[i + j] * BASE**j for j in range(PACK)) for i in range(0, len(jobs), PACK)])
    return slots, packed


def exchange_kernel(
    owner, hidden_ref, gain_ref, wq_ref, wk_ref, all_ref, cols_ref, slots_ref, other_ref, normed_ref, gram_ref,
    n_buf, w_buf, gram, g_buf, c_buf,
    local_sem, recv_sem, send_sem, feed_sem, twin_send, twin_recv, cross_send, cross_recv, load_sem,
):
    tok, col = lax.axis_index("tok"), lax.axis_index("col")
    z, y, core = tok // (WIDE * CORES), tok // CORES % WIDE, tok % CORES
    owner_z, owner_y, owner_core = owner // (WIDE * CORES), owner // CORES % WIDE, owner % CORES
    flip = owner_z >= DEPTH // 2
    owner_at = DEPTH - 1 - owner_z if flip else owner_z
    owner_position = owner_at * WIDE
    key_item = CHIPS + owner_position
    near_z = DEPTH - 1 - z if flip else z
    position = near_z * WIDE + (y + owner_y) % WIDE
    block, features = hidden_ref.shape[0], all_ref.shape[1]
    rows_in_chip = CORES * block
    piece = block // CUT
    head = slots_ref.shape[2]
    depth = slots_ref.shape[1]
    part = depth // CUT
    out_cols = cols_ref.shape[1]
    own_slot, key_slot = CHIPS, CHIPS + 1
    at_owner = position == owner_position
    is_owner = at_owner & (core == owner_core)
    is_fed = at_owner & (core != owner_core)

    def chip_at(where):
        at_z = where // WIDE
        at_z = DEPTH - 1 - at_z if flip else at_z
        return at_z * WIDE + (where % WIDE + owner_y) % WIDE

    def tok_at(where, which):
        return chip_at(where) * CORES + which

    up, down = (tok - WIDE * CORES, tok + WIDE * CORES) if flip else (tok + WIDE * CORES, tok - WIDE * CORES)
    beside = tok + CORES - 2 * CORES * y
    twin = tok + 1 - 2 * core
    partner = 1 - col
    neighbour = (beside, up, down)
    neighbour_position = (position + 1 - 2 * (position % WIDE), position + WIDE, position - WIDE)
    present = (y >= 0, near_z < DEPTH - 1, near_z > 0)

    barrier = pltpu.get_barrier_semaphore()
    for at, there in zip(neighbour, present):
        @pl.when(there)
        def _():
            pl.semaphore_signal(barrier, inc=1, device_id=(at, col), device_id_type=MESH)
    pl.semaphore_signal(barrier, inc=1, device_id=(twin, col), device_id_type=MESH)
    pl.semaphore_signal(barrier, inc=1, device_id=(tok, partner), device_id_type=MESH)
    pl.semaphore_signal(barrier, inc=1, device_id=(twin, partner), device_id_type=MESH)
    take = pltpu.make_async_copy(hidden_ref, n_buf, local_sem.at[0])
    take.start()
    pl.semaphore_wait(barrier, 4 + jnp.minimum(near_z, 1) + jnp.minimum(DEPTH - 1 - near_z, 1))

    def remote(source, target, sent, received, at):
        return pltpu.make_async_remote_copy(
            src_ref=source, dst_ref=target, send_sem=sent, recv_sem=received, device_id=at, device_id_type=MESH
        )

    def rows_of(item, cut):
        return pl.ds(pl.multiple_of(tok_at(item, core) * block + cut * piece, piece), piece)

    def chip_rows(item):
        return pl.ds(pl.multiple_of(chip_at(item) * rows_in_chip, rows_in_chip), rows_in_chip)

    def depth_of(cut):
        return pl.ds(pl.multiple_of(cut * part, part), part)

    def slot_of(item, at):
        where = item - CHIPS
        return jnp.where(item == key_item, key_slot + core, jnp.where(where == at, own_slot, where))

    gives_columns = z // (DEPTH // 2) == col

    def loop(count, body, first=0):
        def step(at, carry):
            body(at)
            return carry

        lax.fori_loop(first, count, step, 0)

    def columns_of(target):
        return pl.ds(pl.multiple_of(target * out_cols % features, out_cols), out_cols)

    def pass_tokens(item, cut):
        rows = rows_of(item, cut)
        remote(all_ref.at[rows], all_ref.at[rows], twin_send.at[0], twin_recv.at[item], (twin, col)).start()

        @pl.when(gives_columns)
        def _():
            def give(which):
                target = tok - core + which
                remote(
                    all_ref.at[rows, columns_of(target)], cols_ref.at[rows], cross_send.at[0],
                    cross_recv.at[core * CHIPS + item], (target, partner),
                ).start()

            loop(CORES, give)

    def pass_keys(cut):
        ref = slots_ref.at[key_slot + core, depth_of(cut)]
        remote(ref, ref, twin_send.at[1], twin_recv.at[CHIPS], (twin, col)).start()

    def pass_weights(cut):
        @pl.when(cut // (CUT // 2) == partner)
        def _():
            remote(
                slots_ref.at[own_slot, depth_of(cut)],
                other_ref.at[pl.ds(pl.multiple_of(cut % (CUT // 2) * part, part), part)],
                cross_send.at[1], cross_recv.at[CORES * CHIPS], (tok, partner),
            ).start()

    order, keys_at, key_step = [], 0, 0
    for step in range(len(step_entries(owner_at, 0, 0))):
        for direction in (1, 0, 2):
            entry = step_entries(owner_at, direction, owner_position)[step]
            item = (entry - 1) // CUT - CHIPS
            if item == owner_position and not keys_at:
                keys_at, key_step = len(order), step
            elif entry and item >= 0 and item not in order and item != owner_position:
                order.append(item)
    order.append(owner_position)
    fed_core = 1 - owner_core

    def feed(item, cut):
        lane = pl.multiple_of(tok_at(item, fed_core) * head, head)
        slot = jnp.where(item == owner_position, own_slot, item)
        return remote(
            wq_ref.at[0, depth_of(cut), pl.ds(lane, head)], slots_ref.at[slot, depth_of(cut)],
            feed_sem.at[0, item * CUT + cut], feed_sem.at[1, item * CUT + cut], (twin, col),
        )

    def feed_keys(cut):
        return remote(
            wk_ref.at[0, depth_of(cut), pl.ds(fed_core * head, head)],
            slots_ref.at[key_slot + fed_core, depth_of(cut)],
            feed_sem.at[0, CHIPS * CUT + cut], feed_sem.at[1, CHIPS * CUT + cut], (twin, col),
        )

    def feed_some(first, last):
        loop((last - first) * CUT, lambda at: feed(choose(at // CUT + first, order), at % CUT).start())

    @pl.when(is_owner)
    def _():
        feed_some(0, keys_at)
        loop(CUT, lambda cut: feed_keys(cut).start())
        feed_some(keys_at, CHIPS)

    def through(source, buffer, target, sem):
        take = pltpu.make_async_copy(source, buffer, sem)
        take.start()
        take.wait()
        put = pltpu.make_async_copy(buffer, target, sem)
        put.start()
        put.wait()

    take.wait()
    strip, few = 16, 32

    def normalize_strip(at):
        some = pl.ds(pl.multiple_of(at * strip, strip), strip)
        wide = n_buf[some, :].astype(jnp.float32)
        meansq = jnp.sum(wide * wide, axis=1, keepdims=True) / wide.shape[1]
        n_buf[some, :] = (wide * lax.rsqrt(meansq + 1e-05) * gain_ref[...]).astype(n_buf.dtype)

    loop(block // strip, normalize_strip)

    @pl.when(is_owner)
    def _():
        through(
            wk_ref.at[0, :, pl.ds(owner_core * head, head)], w_buf, slots_ref.at[key_slot + owner_core], local_sem.at[1]
        )
        through(wq_ref.at[0, :, pl.ds(owner * head, head)], w_buf, slots_ref.at[own_slot], local_sem.at[1])

    put = pltpu.make_async_copy(
        n_buf.at[:, pl.ds(pl.multiple_of(col * features, features), features)],
        all_ref.at[pl.ds(pl.multiple_of(tok * block, block), block)], local_sem.at[0],
    )
    put.start()
    keep = pltpu.make_async_copy(n_buf, normed_ref, local_sem.at[2])
    keep.start()

    def clear(at):
        gram[pl.ds(pl.multiple_of(at * few, few), few), :] = jnp.zeros((few, out_cols), jnp.float32)

    loop(features // few, clear)
    put.wait()

    @pl.when(is_owner)
    def _():
        loop(CUT, pass_keys)
        loop(CUT, pass_weights)

    loop(CUT, lambda cut: pass_tokens(position, cut))

    tables = [[packed_table(owner_at, direction, late) for direction in range(3)] for late in (False, True)]
    length = len(tables[0][0][0])
    mine = [
        [
            choose(position, [tables[late][direction][p][i] for p in range(CHIPS)])
            for direction in range(3)
            for i in range(length)
        ]
        for late in range(2)
    ]

    def entry_at(late, direction, step):
        number = choose(direction * length + step // PACK, mine[late])
        return number // choose(step % PACK, [BASE**j for j in range(PACK)]) % BASE

    slots, job_numbers = job_table(owner_at)
    my_jobs = [choose(position, [job_numbers[p][i] for p in range(CHIPS)]) for i in range(len(job_numbers[0]))]

    def job_at(slot):
        return choose(slot // PACK, my_jobs) // choose(slot % PACK, [BASE**j for j in range(PACK)]) % BASE

    def wait_remote(ref, sem):
        remote(ref, ref, twin_send.at[0], sem, (twin, col)).wait_recv()

    def load_block(item, slot):
        return pltpu.make_async_copy(all_ref.at[chip_rows(item)], g_buf.at[slot % 2], load_sem.at[0, slot % 2])

    def load_columns(source, slot):
        return pltpu.make_async_copy(source, c_buf.at[slot % 2], load_sem.at[1, slot % 2])

    def slot_body(slot):
        item = job_at(slot) - 1

        @pl.when(item >= 0)
        def _():
            wait_remote(all_ref.at[pl.ds(0, block)], twin_recv.at[item])
            load_block(item, slot).start()

            @pl.when(gives_columns)
            def _():
                load_columns(all_ref.at[chip_rows(item), columns_of(tok)], slot).start()

            @pl.when(jnp.logical_not(gives_columns))
            def _():
                for which in range(CORES):
                    wait_remote(cols_ref.at[pl.ds(0, block)], cross_recv.at[which * CHIPS + item])
                load_columns(cols_ref.at[chip_rows(item)], slot).start()

        before = job_at(slot - 1) - 1
        at = (slot + 1) % 2

        @pl.when(before >= 0)
        def _():
            load_block(before, slot - 1).wait()
            load_columns(cols_ref.at[pl.ds(0, rows_in_chip)], slot - 1).wait()
            tile = out_cols // 2

            def term(some):
                lanes = pl.ds(pl.multiple_of(some * tile, tile), tile)
                gram[lanes, :] += lax.dot_general(
                    g_buf[at, :, lanes], c_buf[at], (((0,), (0,)), ((), ())), preferred_element_type=jnp.float32
                )

            loop(features // tile, term)

    def arrived(entry):
        item, cut = (entry - 1) // CUT, (entry - 1) % CUT
        rows = rows_of(0, 0)
        remote(all_ref.at[rows], all_ref.at[rows], send_sem.at[0, 0], recv_sem.at[entry - 1], (twin, col)).wait_recv()

        @pl.when(item < CHIPS)
        def _():
            pass_tokens(item, cut)

        @pl.when(item == key_item)
        def _():
            pass_keys(cut)

        @pl.when((item == position + CHIPS) & (item != key_item))
        def _():
            pass_weights(cut)

    def send(source, target, direction, entry, step):
        return remote(
            source, target, send_sem.at[direction, step], recv_sem.at[entry - 1], (choose(direction, neighbour), col)
        )

    def send_tokens(direction, entry, step):
        rows = rows_of((entry - 1) // CUT, (entry - 1) % CUT)
        return send(all_ref.at[rows], all_ref.at[rows], direction, entry, step)

    def send_weights(direction, entry, step, stored):
        item, cut = (entry - 1) // CUT, (entry - 1) % CUT
        target = slots_ref.at[slot_of(item, choose(direction, neighbour_position)), depth_of(cut)]
        lane = pl.multiple_of(tok_at(item - CHIPS, core) * head, head)
        if stored:
            source = wq_ref.at[0, depth_of(cut), pl.ds(lane, head)]
        else:
            source = slots_ref.at[slot_of(item, position), depth_of(cut)]
        return send(source, target, direction, entry, step)

    def fed(at):
        ref = slots_ref.at[own_slot, depth_of(0)]
        remote(ref, ref, feed_sem.at[0, at], feed_sem.at[1, at], (twin, col)).wait_recv()

    head_step = 8

    def step_body(step):
        @pl.when(is_fed & (step == key_step))
        def _():
            def take(cut):
                fed(CHIPS * CUT + cut)
                pass_keys(cut)

            loop(CUT, take)

        @pl.when(is_fed & (step == head_step))
        def _():
            def take(cut):
                fed(owner_position * CUT + cut)
                pass_weights(cut)

            loop(CUT, take)

        def receive(direction):
            entry = entry_at(1, direction, step)

            @pl.when(entry > 0)
            def _():
                arrived(entry)

        loop(3, receive)

        def forward(direction):
            entry = entry_at(0, direction, step)
            item = (entry - 1) // CUT
            stored = is_owner & (item != key_item)

            @pl.when((entry > 0) & (item < CHIPS))
            def _():
                send_tokens(direction, entry, step).start()

            @pl.when((item >= CHIPS) & is_fed & (item != key_item))
            def _():
                fed(entry - 1 - CHIPS * CUT)

            @pl.when((item >= CHIPS) & stored)
            def _():
                send_weights(direction, entry, step, True).start()

            @pl.when((item >= CHIPS) & jnp.logical_not(stored))
            def _():
                send_weights(direction, entry, step, False).start()

        loop(3, forward)
        loop(SLOTS * step + SLOTS, slot_body, SLOTS * step)

    steps = length * PACK
    loop(steps, step_body)
    loop(max(slots + 1, SLOTS * steps), slot_body, SLOTS * steps)
    store = pltpu.make_async_copy(gram, gram_ref, local_sem.at[1])
    store.start()

    def drain(at):
        step, direction = at // 3, at % 3

        @pl.when(entry_at(0, direction, step) > 0)
        def _():
            send_tokens(direction, jnp.int32(1), step).wait_send()

    loop(3 * steps, drain)

    @pl.when(is_owner)
    def _():
        loop(CHIPS * CUT, lambda at: feed(at // CUT, at % CUT).wait_send())
        loop(CUT, lambda cut: feed_keys(cut).wait_send())

    halves = all_ref.at[pl.ds(0, all_ref.shape[0] // CORES)]
    remote(halves, halves, twin_send.at[0], twin_recv.at[0], (twin, col)).wait_send()
    keys = slots_ref.at[key_slot]
    remote(keys, keys, twin_send.at[1], twin_recv.at[CHIPS], (twin, col)).wait()
    remote(other_ref, other_ref, cross_send.at[1], cross_recv.at[CORES * CHIPS], (tok, partner)).wait()

    @pl.when(gives_columns)
    def _():
        remote(cols_ref, cols_ref, cross_send.at[0], cross_recv.at[0], (tok, partner)).wait_send()

    keep.wait()
    store.wait()


def exchange(owner, hidden, gain, wq, wk):
    block, width = hidden.shape
    groups = CHIPS * CORES
    features = width // lax.axis_size("col")
    depth = wq.shape[1]
    head = wk.shape[2] // CORES
    out_cols = width // groups
    rows = CORES * block
    steps = max(send_steps(owner_at) for owner_at in range(len(ROUTES)))
    kind, wide = hidden.dtype, jnp.float32
    any_space = pl.BlockSpec(memory_space=pl.ANY)
    vmem = pl.BlockSpec(memory_space=pltpu.VMEM)
    gathered, _, slots, other, normed, gram = pl.pallas_call(
        functools.partial(exchange_kernel, owner),
        out_shape=(
            jax.ShapeDtypeStruct((groups * block, features), kind),
            jax.ShapeDtypeStruct((groups * block, out_cols), kind),
            jax.ShapeDtypeStruct((CHIPS + 3, depth, head), kind),
            jax.ShapeDtypeStruct((depth // 2, head), kind),
            jax.ShapeDtypeStruct((block, width), kind),
            jax.ShapeDtypeStruct((features, out_cols), wide),
        ),
        in_specs=[any_space, vmem, any_space, any_space],
        out_specs=(any_space,) * 6,
        scratch_shapes=[
            pltpu.VMEM((block, width), kind),
            pltpu.VMEM((depth, head), kind),
            pltpu.VMEM((features, out_cols), wide),
            pltpu.VMEM((2, rows, features), kind),
            pltpu.VMEM((2, rows, out_cols), kind),
            pltpu.SemaphoreType.DMA((3,)),
            pltpu.SemaphoreType.DMA((2 * CHIPS * CUT,)),
            pltpu.SemaphoreType.DMA((3, steps)),
            pltpu.SemaphoreType.DMA((2, (CHIPS + 1) * CUT)),
            pltpu.SemaphoreType.DMA((2,)),
            pltpu.SemaphoreType.DMA((CHIPS + 1,)),
            pltpu.SemaphoreType.DMA((2,)),
            pltpu.SemaphoreType.DMA((CORES * CHIPS + 1,)),
            pltpu.SemaphoreType.DMA((2, 2)),
        ],
        compiler_params=pltpu.CompilerParams(collective_id=owner, has_side_effects=True),
    )(hidden, gain, wq, wk)
    return gathered, slots, other, normed, gram


def finish_kernel(
    all_ref, slots_ref, other_ref, normed_ref, cos_ref, sin_ref, q_ref, k_ref,
    w_buf, g_buf, n_buf, kw_buf, acc, own_buf, part_buf, part_recv, sum_buf, heads,
    load_sem, w_sem, part_sem, sum_sem, head_sem, keep_sem,
):
    tok, col = lax.axis_index("tok"), lax.axis_index("col")
    groups = CHIPS * CORES
    chip, partner = tok // CORES, 1 - col
    features, head = other_ref.shape
    rows = all_ref.shape[0] // CHIPS
    block = rows // CORES
    depth = slots_ref.shape[1]
    key_slot = CHIPS + 1

    def loop(count, body, first=0):
        def step(at, carry):
            body(at)
            return carry

        lax.fori_loop(first, count, step, 0)

    barrier = pltpu.get_barrier_semaphore()

    def greet(at):
        pl.semaphore_signal(barrier, inc=1, device_id=(lax.rem(tok + at, groups), col), device_id_type=MESH)

    loop(groups, greet, 1)
    pl.semaphore_signal(barrier, inc=1, device_id=(tok, partner), device_id_type=MESH)

    def load(at):
        where = lax.rem(chip + 1 + at, CHIPS)
        return pltpu.make_async_copy(
            all_ref.at[pl.ds(pl.multiple_of(where * rows, rows), rows)], g_buf.at[at % 2], load_sem.at[at % 2]
        )

    own = pltpu.make_async_copy(
        slots_ref.at[CHIPS, pl.ds(pl.multiple_of(col * features, features), features)],
        w_buf.at[:, pl.ds(0, head)], w_sem.at[0],
    )
    own.start()
    crossed = pltpu.make_async_copy(other_ref, w_buf.at[:, pl.ds(head, head)], w_sem.at[1])
    crossed.start()
    load(0).start()
    later = [pltpu.make_async_copy(normed_ref, n_buf, w_sem.at[2])]
    for which in range(CORES):
        later.append(
            pltpu.make_async_copy(
                slots_ref.at[key_slot + which], kw_buf.at[:, pl.ds(which * head, head)], w_sem.at[3 + which]
            )
        )
    own.wait()
    crossed.wait()

    def cross(at):
        return pltpu.make_async_remote_copy(
            src_ref=part_buf.at[at], dst_ref=part_recv.at[at], send_sem=part_sem.at[0, at], recv_sem=part_sem.at[1, at],
            device_id=(tok, partner), device_id_type=MESH,
        )

    def hand(at, which):
        source = sum_buf.at[at, pl.ds(which * block, block)]
        target = lax.rem(chip + 1 + at, CHIPS) * CORES + which
        away = pltpu.make_async_remote_copy(
            src_ref=source, dst_ref=heads.at[tok], send_sem=sum_sem.at[at, which], recv_sem=head_sem.at[0],
            device_id=(target, col), device_id_type=MESH,
        )
        return target, away, pltpu.make_async_copy(source, heads.at[tok], keep_sem.at[0])

    even = lax.broadcasted_iota(jnp.int32, (block, head), 1) % 2 == 0

    def turned(raw):
        swapped = jnp.where(even, pltpu.roll(raw, head - 1, 1), pltpu.roll(raw, 1, 1))
        return raw * cos_ref[...] + swapped * sin_ref[...]

    tile = Q_TILE
    def query(at):
        acc[...] = jnp.zeros(acc.shape, jnp.float32)

        def term(some):
            lanes = pl.ds(pl.multiple_of(some * tile, tile), tile)
            acc[...] += jnp.dot(g_buf[at % 2, :, lanes], w_buf[lanes, :], preferred_element_type=jnp.float32)

        loop(features // tile, term)
        own_buf[at] = acc[:, :head]
        part_buf[at] = acc[:, head:].astype(part_buf.dtype)

    def key():
        some_acc = acc.at[pl.ds(0, block)]
        some_acc[...] = jnp.zeros(some_acc.shape, jnp.float32)

        def term(some):
            lanes = pl.ds(pl.multiple_of(some * tile, tile), tile)
            some_acc[...] += jnp.dot(n_buf[:, lanes], kw_buf[lanes, :], preferred_element_type=jnp.float32)

        loop(depth // tile, term)

        def finish_key(which):
            lanes = pl.ds(pl.multiple_of(which * head, head), head)
            k_ref[:, lanes] = turned(some_acc[:, lanes]).astype(k_ref.dtype)

        loop(CORES, finish_key)

    hand_lag, sum_lag = 3, 2

    def body(at):
        @pl.when(at < CHIPS)
        def _():
            load(at).wait()

        @pl.when(at + 1 < CHIPS)
        def _():
            load(at + 1).start()

        @pl.when(at == 0)
        def _():
            for copy in later:
                copy.start()
            pl.semaphore_wait(barrier, groups)

        @pl.when((at >= 1) & (at < CHIPS + 1))
        def _():
            cross(at - 1).start()

        @pl.when((at >= hand_lag) & (at < CHIPS + hand_lag))
        def _():
            for which in range(CORES):
                target, away, keep = hand(at - hand_lag, which)

                @pl.when(target != tok)
                def _():
                    away.start()

                @pl.when(target == tok)
                def _():
                    keep.start()

        @pl.when(at < CHIPS)
        def _():
            query(at)

        @pl.when(at == CHIPS)
        def _():
            for copy in later:
                copy.wait()
            key()

        @pl.when((at >= sum_lag) & (at < CHIPS + sum_lag))
        def _():
            done = at - sum_lag
            cross(done).wait_recv()
            sum_buf[done] = (own_buf[done] + part_recv[done].astype(jnp.float32)).astype(sum_buf.dtype)

    loop(CHIPS + hand_lag, body)

    def drain(at):
        cross(at).wait_send()
        for which in range(CORES):
            target, away, keep = hand(at, which)

            @pl.when(target != tok)
            def _():
                away.wait_send()

            @pl.when(target == tok)
            def _():
                keep.wait()

    loop(CHIPS, drain)
    others = heads.at[pl.ds(0, groups - 1)]
    pltpu.make_async_remote_copy(
        src_ref=others, dst_ref=others, send_sem=sum_sem.at[0, 0], recv_sem=head_sem.at[0],
        device_id=(tok, partner), device_id_type=MESH,
    ).wait_recv()

    def finish_head(at):
        lanes = pl.ds(pl.multiple_of(at * head, head), head)
        q_ref[:, lanes] = turned(heads[at].astype(jnp.float32)).astype(q_ref.dtype)

    loop(groups, finish_head)


Q_TILE = 1024


def finish(gathered, slots, other, normed, cosine, sine):
    features, head = other.shape
    groups = CHIPS * CORES
    rows = gathered.shape[0] // CHIPS
    block = rows // CORES
    depth = slots.shape[1]
    kind, wide = gathered.dtype, jnp.float32
    any_space = pl.BlockSpec(memory_space=pl.ANY)
    vmem = pl.BlockSpec(memory_space=pltpu.VMEM)
    return pl.pallas_call(
        finish_kernel,
        out_shape=(
            jax.ShapeDtypeStruct((block, groups * head), kind),
            jax.ShapeDtypeStruct((block, CORES * head), kind),
        ),
        in_specs=[any_space] * 4 + [vmem] * 2,
        out_specs=(vmem, vmem),
        scratch_shapes=[
            pltpu.VMEM((features, 2 * head), kind),
            pltpu.VMEM((2, rows, features), kind),
            pltpu.VMEM((block, depth), kind),
            pltpu.VMEM((depth, CORES * head), kind),
            pltpu.VMEM((rows, 2 * head), wide),
            pltpu.VMEM((CHIPS, rows, head), wide),
            pltpu.VMEM((CHIPS, rows, head), kind),
            pltpu.VMEM((CHIPS, rows, head), kind),
            pltpu.VMEM((CHIPS, rows, head), kind),
            pltpu.VMEM((groups, block, head), kind),
            pltpu.SemaphoreType.DMA((2,)),
            pltpu.SemaphoreType.DMA((3 + CORES,)),
            pltpu.SemaphoreType.DMA((2, CHIPS)),
            pltpu.SemaphoreType.DMA((CHIPS, CORES)),
            pltpu.SemaphoreType.DMA((1,)),
            pltpu.SemaphoreType.DMA((1,)),
        ],
        compiler_params=pltpu.CompilerParams(collective_id=groups, has_side_effects=True),
    )(gathered, slots, other, normed, cosine, sine)


def angles(place):
    dims = jnp.arange(HEAD, dtype=jnp.int32)
    pair = (dims // 2).astype(jnp.float32)
    freq = jnp.power(jnp.float32(rope_base), -2.0 * pair / HEAD)
    angle = place.astype(jnp.float32)[:, None] * freq[None, :]
    sine = jnp.where((dims % 2 == 0)[None, :], -jnp.sin(angle), jnp.sin(angle))
    return jnp.cos(angle), sine


def grid_shards(hidden, norm_gain, token_ids, owner, query_store, key_store):
    cosine, sine = lax.optimization_barrier(angles(positions(token_ids)))
    groups = lax.axis_size("tok")
    branches = [functools.partial(exchange, at) for at in range(groups)]
    gathered, slots, other, normed, gram = lax.switch(owner[0], branches, hidden, norm_gain[None, :], query_store, key_store)
    queries, keys = finish(gathered, slots, other, normed, cosine, sine)
    return (queries, keys, gram * (2.0 / (hidden.shape[0] * groups)))


def solution(mesh):
    placed = (P("tok", None), P(), P("tok"), P(), P("tok", None, "col"), P("tok", None, "col"))
    fits = mesh.shape["tok"] == CHIPS * CORES and mesh.shape["col"] == 2
    return jax.shard_map(
        grid_shards if fits else shards,
        mesh=mesh,
        in_specs=placed,
        out_specs=(P("tok", "col"), P("tok", "col"), P("col", "tok")),
        check_vma=False,
    )
```

```python
import functools

import jax
import jax.numpy as jnp
from jax import lax
from jax.experimental import pallas as pl
from jax.experimental.pallas import tpu as pltpu
from jax.sharding import PartitionSpec as P

HEAD = 128
SEQ = 128


begin_token = 128000
rope_base = 500000.0


def scatter_weights(query, key, owner):
    groups = lax.axis_size("tok")
    depth, width = query.shape
    piece = width // groups
    mine = lax.axis_index("tok") == owner
    query = jnp.moveaxis(query.reshape(depth, groups, piece), 1, 0)
    key = key.reshape(groups, depth * key.shape[1] // groups // piece, piece)
    both = jnp.concatenate([query, key], axis=1)
    return jnp.where(mine, both, jnp.zeros_like(both))


def positions(token_ids):
    samples = token_ids.reshape(-1, SEQ)
    index = jnp.arange(SEQ, dtype=jnp.int32)
    starts = jnp.where(samples == begin_token, index[None, :], jnp.zeros_like(samples))
    latest = lax.cummax(starts, axis=1)
    return (index[None, :] - latest).reshape(-1)


def rotate(values, place, start):
    width = values.shape[1]
    period = HEAD if width % HEAD == 0 else width
    dims = (start + jnp.arange(period, dtype=jnp.int32)) % HEAD
    pair = (dims // 2).astype(jnp.float32)
    freq = jnp.power(jnp.float32(rope_base), -2.0 * pair / HEAD)
    angle = place.astype(jnp.float32)[:, None] * freq[None, :]
    even = dims % 2 == 0
    sine = jnp.where(even[None, :], -jnp.sin(angle), jnp.sin(angle))
    cosine, sine = lax.optimization_barrier((jnp.cos(angle), sine))
    cosine = jnp.tile(cosine, (1, width // period))
    sine = jnp.tile(sine, (1, width // period))
    following = jnp.concatenate([values[:, 1:], values[:, :1]], axis=1)
    previous = jnp.concatenate([values[:, -1:], values[:, :-1]], axis=1)
    even = jnp.arange(width, dtype=jnp.int32) % 2 == 0
    other = jnp.where(even[None, :], following, previous)
    return values * cosine + other * sine


def normalize(hidden, norm_gain):
    wide = hidden.astype(jnp.float32)
    meansq = jnp.mean(wide * wide, axis=-1, keepdims=True)
    return (wide * lax.rsqrt(meansq + 1e-05) * norm_gain[None, :]).astype(jnp.bfloat16)


def transposed_product(left, right):
    return lax.dot_general(
        left, right, (((0,), (0,)), ((), ())), preferred_element_type=jnp.float32
    )


def shards(hidden, norm_gain, token_ids, owner, query_store, key_store):
    normed = normalize(hidden, norm_gain)
    place = positions(token_ids)
    column = lax.axis_index("col")
    row_width = normed.shape[1] // lax.axis_size("col")
    row_block = lax.dynamic_slice_in_dim(normed, column * row_width, row_width, 1)
    total_tokens = normed.shape[0] * lax.axis_size("tok")
    groups, parts = lax.axis_size("tok"), lax.axis_size("col")
    depth, q_width = query_store.shape[1:]
    k_width = key_store.shape[2]
    masked = scatter_weights(query_store[0], key_store[0], owner[0])
    gathered = lax.all_gather(row_block, "tok", axis=0, tiled=True)
    col_block = lax.all_to_all(normed, "tok", split_axis=1, concat_axis=0, tiled=True)
    masked, gathered = lax.optimization_barrier((masked, gathered))
    owned = lax.psum_scatter(masked, "tok", scatter_dimension=0, tiled=False)
    gram = transposed_product(gathered, col_block)
    hessian = gram * (2.0 / total_tokens)
    key_rows = owned[depth:].reshape(depth // groups, k_width)
    weight_k = lax.all_gather(key_rows, "tok", axis=0, tiled=True)
    weight_q = lax.all_to_all(owned[:depth], "col", split_axis=0, concat_axis=1, tiled=True)
    partial = jnp.dot(gathered, weight_q, preferred_element_type=jnp.float32).astype(jnp.bfloat16)
    partial = lax.all_to_all(partial, "col", split_axis=1, concat_axis=0, tiled=True)
    partial = partial.reshape(parts, total_tokens, q_width // groups).astype(jnp.float32)
    summed = jnp.sum(partial, axis=0).astype(jnp.bfloat16)
    raw_q = lax.all_to_all(summed, "tok", split_axis=0, concat_axis=1, tiled=True).astype(jnp.float32)
    raw_k = jnp.dot(normed, weight_k, preferred_element_type=jnp.float32)
    queries = rotate(raw_q, place, column * q_width).astype(jnp.bfloat16)
    keys = rotate(raw_k, place, column * k_width).astype(jnp.bfloat16)
    return (queries, keys, hessian)


MESH = pl.DeviceIdType.MESH

DEPTH, WIDE, CORES = 4, 2, 2
CHIPS = DEPTH * WIDE
CUT = 4
LAG = 2
BASE = 128
PACK = 4
ROUTES = (
    (
        (
            (76078909, 8438017, 114118945, 80303143, 25347337),
            (29573893, 42255367, 4127, 0, 0),
            (38028553, 25349401, 97213495, 6191, 0),
            (29575183, 76071685, 8438017, 16896031, 0),
            (38029843, 25354303, 76074265, 8438017, 0),
            (29575957, 21122071, 33800965, 71843840, 1031),
            (38030875, 29575957, 3353, 4215331, 25346563),
            (67620637, 21121555, 3095, 33800965, 16896289),
        ),
        (
            (126804031, 118349113, 101439277, 109893937, 88757803),
            (131023621, 4215331, 71844355, 114115591, 0),
            (135251467, 122576443, 4215331, 105660931, 6707),
            (21120781, 12672829, 118343695, 16896289, 6965),
            (46483729, 126797581, 76078393, 8438017, 1547),
            (42257431, 135251209, 12672829, 71845903, 1031),
            (0, 0, 0, 0, 0),
            (0, 0, 0, 0, 0),
        ),
        (
            (0, 0, 0, 0, 0),
            (0, 0, 0, 0, 0),
            (25347337, 46483729, 63393307, 33803287, 3353),
            (46483213, 67619347, 63393307, 38030359, 54937615),
            (54937873, 59165461, 50712349, 2579, 4385),
            (42257173, 59166751, 50712349, 0, 0),
            (59165977, 67620637, 0, 0, 0),
            (59166751, 3869, 0, 0, 0),
        ),
    ),
    (
        (
            (88752385, 8443435, 21121555, 25349143, 3353),
            (29573893, 46483471, 63393307, 16894225, 4127),
            (84533053, 118346533, 101439277, 25347337, 0),
            (50710285, 16893967, 12668701, 4127, 0),
            (135252241, 42254851, 21122329, 114116107, 0),
            (29575957, 4211719, 92982295, 33800965, 0),
            (42257947, 29575441, 4211977, 54937099, 1031),
            (67620637, 50711317, 88752643, 12670507, 2063),
        ),
        (
            (4211203, 0, 0, 0, 0),
            (4211719, 92984617, 8438533, 0, 0),
            (8446015, 25347337, 122576443, 105667381, 6707),
            (16893709, 88752385, 12670507, 131024911, 7223),
            (38029843, 21120781, 25346305, 126796807, 7481),
            (50711317, 8446015, 92984617, 33800965, 7997),
            (0, 0, 0, 0, 0),
            (0, 0, 0, 0, 0),
        ),
        (
            (0, 0, 0, 0, 0),
            (0, 0, 0, 0, 0),
            (92984617, 21121555, 25349143, 76074265, 4385),
            (33801997, 59165461, 38031133, 84529183, 4901),
            (54938131, 59165461, 2321, 0, 0),
            (46484503, 63393307, 67619089, 54938131, 0),
            (59165977, 67620637, 0, 5417, 0),
            (59166493, 4127, 0, 0, 0),
        ),
    ),
)


def step_entries(owner_at, direction, position):
    entries = []
    for number in ROUTES[owner_at][direction][position]:
        for _ in range(PACK):
            entries.append(number % BASE)
            number //= BASE
    return entries


def packed_table(owner_at, direction, arrivals):
    table = []
    for position in range(CHIPS):
        entries = None
        if not arrivals:
            entries = step_entries(owner_at, direction, position) + [0] * LAG
        else:
            z = position // WIDE + (0, -1, 1)[direction]
            sender = position ^ 1 if direction == 0 else z * WIDE + position % WIDE
            entries = [0] * LAG + (
                step_entries(owner_at, direction, sender) if 0 <= z < DEPTH else [0] * len(step_entries(owner_at, 0, 0))
            )
        entries += [0] * (-len(entries) % PACK)
        table.append([
            sum(entries[i + j] * BASE**j for j in range(PACK)) for i in range(0, len(entries), PACK)
        ])
    return table


def choose(index, options):
    value = jnp.int32(0)
    for at, option in enumerate(options):
        if isinstance(option, int) and option == 0:
            continue
        value = jnp.where(index == at, jnp.int32(option) if isinstance(option, int) else option, value)
    return value


def arrival_steps(owner_at):
    steps = [[None] * (2 * CHIPS) for _ in range(CHIPS)]
    for position in range(CHIPS):
        for direction in range(3):
            z = position // WIDE + (0, 1, -1)[direction]
            target = position ^ 1 if direction == 0 else z * WIDE + position % WIDE
            for step, entry in enumerate(step_entries(owner_at, direction, position)):
                if entry:
                    item = (entry - 1) // CUT
                    steps[target][item] = max(steps[target][item] or 0, step + LAG)
    return steps


SLOTS = 2


def send_steps(owner_at):
    return (len(step_entries(owner_at, 0, 0)) + LAG + PACK - 1) // PACK * PACK


def job_table(owner_at):
    table = []
    for position, steps in enumerate(arrival_steps(owner_at)):
        ready = [1 if item == position else steps[item] + 1 for item in range(CHIPS)]
        waiting = sorted(range(CHIPS), key=lambda item: (ready[item], item))
        jobs = []
        while waiting:
            step = len(jobs) // SLOTS
            jobs.append(waiting.pop(0) + 1 if ready[waiting[0]] <= step else 0)
        table.append(jobs)
    slots = max(len(jobs) for jobs in table)
    packed = []
    for jobs in table:
        jobs = jobs + [0] * (-slots % PACK + slots - len(jobs))
        packed.append([sum(jobs[i + j] * BASE**j for j in range(PACK)) for i in range(0, len(jobs), PACK)])
    return slots, packed, [len(jobs) - 1 for jobs in table]


def exchange_kernel(
    owner, hidden_ref, gain_ref, wq_ref, wk_ref, all_ref, cols_ref, slots_ref, other_ref, normed_ref, gram_ref,
    n_buf, w_buf, gram, g_buf, c_buf,
    local_sem, recv_sem, send_sem, feed_sem, twin_send, twin_recv, cross_send, cross_recv, load_sem,
):
    tok, col = lax.axis_index("tok"), lax.axis_index("col")
    z, y, core = tok // (WIDE * CORES), tok // CORES % WIDE, tok % CORES
    owner_z, owner_y, owner_core = owner // (WIDE * CORES), owner // CORES % WIDE, owner % CORES
    flip = owner_z >= DEPTH // 2
    owner_at = DEPTH - 1 - owner_z if flip else owner_z
    owner_position = owner_at * WIDE
    key_item = CHIPS + owner_position
    near_z = DEPTH - 1 - z if flip else z
    position = near_z * WIDE + (y + owner_y) % WIDE
    block, features = hidden_ref.shape[0], all_ref.shape[1]
    rows_in_chip = CORES * block
    piece = block // CUT
    head = slots_ref.shape[2]
    depth = slots_ref.shape[1]
    part = depth // CUT
    out_cols = cols_ref.shape[1]
    own_slot, key_slot = CHIPS, CHIPS + 1
    at_owner = position == owner_position
    is_owner = at_owner & (core == owner_core)
    is_fed = at_owner & (core != owner_core)

    def chip_at(where):
        at_z = where // WIDE
        at_z = DEPTH - 1 - at_z if flip else at_z
        return at_z * WIDE + (where % WIDE + owner_y) % WIDE

    def tok_at(where, which):
        return chip_at(where) * CORES + which

    up, down = (tok - WIDE * CORES, tok + WIDE * CORES) if flip else (tok + WIDE * CORES, tok - WIDE * CORES)
    beside = tok + CORES - 2 * CORES * y
    twin = tok + 1 - 2 * core
    partner = 1 - col
    neighbour = (beside, up, down)
    neighbour_position = (position + 1 - 2 * (position % WIDE), position + WIDE, position - WIDE)
    present = (y >= 0, near_z < DEPTH - 1, near_z > 0)

    barrier = pltpu.get_barrier_semaphore()
    for at, there in zip(neighbour, present):
        @pl.when(there)
        def _():
            pl.semaphore_signal(barrier, inc=1, device_id=(at, col), device_id_type=MESH)
    pl.semaphore_signal(barrier, inc=1, device_id=(twin, col), device_id_type=MESH)
    pl.semaphore_signal(barrier, inc=1, device_id=(tok, partner), device_id_type=MESH)
    pl.semaphore_signal(barrier, inc=1, device_id=(twin, partner), device_id_type=MESH)
    take = pltpu.make_async_copy(hidden_ref, n_buf, local_sem.at[0])
    take.start()
    pl.semaphore_wait(barrier, 4 + jnp.minimum(near_z, 1) + jnp.minimum(DEPTH - 1 - near_z, 1))

    def remote(source, target, sent, received, at):
        return pltpu.make_async_remote_copy(
            src_ref=source, dst_ref=target, send_sem=sent, recv_sem=received, device_id=at, device_id_type=MESH
        )

    def rows_of(item, cut):
        return pl.ds(pl.multiple_of(tok_at(item, core) * block + cut * piece, piece), piece)

    def chip_rows(item):
        return pl.ds(pl.multiple_of(chip_at(item) * rows_in_chip, rows_in_chip), rows_in_chip)

    def depth_of(cut):
        return pl.ds(pl.multiple_of(cut * part, part), part)

    def slot_of(item, at):
        where = item - CHIPS
        return jnp.where(item == key_item, key_slot + core, jnp.where(where == at, own_slot, where))

    gives_columns = z // (DEPTH // 2) == col

    def loop(count, body, first=0):
        def step(at, carry):
            body(at)
            return carry

        lax.fori_loop(first, count, step, 0)

    def columns_of(target):
        return pl.ds(pl.multiple_of(target * out_cols % features, out_cols), out_cols)

    def pass_tokens(item, cut):
        rows = rows_of(item, cut)
        remote(all_ref.at[rows], all_ref.at[rows], twin_send.at[0], twin_recv.at[item], (twin, col)).start()

        @pl.when(gives_columns)
        def _():
            def give(which):
                target = tok - core + which
                remote(
                    all_ref.at[rows, columns_of(target)], cols_ref.at[rows], cross_send.at[0],
                    cross_recv.at[core * CHIPS + item], (target, partner),
                ).start()

            loop(CORES, give)

    def pass_keys(cut):
        ref = slots_ref.at[key_slot + core, depth_of(cut)]
        remote(ref, ref, twin_send.at[1], twin_recv.at[CHIPS], (twin, col)).start()

    def pass_weights(cut):
        @pl.when(cut // (CUT // 2) == partner)
        def _():
            remote(
                slots_ref.at[own_slot, depth_of(cut)],
                other_ref.at[pl.ds(pl.multiple_of(cut % (CUT // 2) * part, part), part)],
                cross_send.at[1], cross_recv.at[CORES * CHIPS], (tok, partner),
            ).start()

    order, keys_at, key_step = [], 0, 0
    for step in range(len(step_entries(owner_at, 0, 0))):
        for direction in (1, 0, 2):
            entry = step_entries(owner_at, direction, owner_position)[step]
            item = (entry - 1) // CUT - CHIPS
            if item == owner_position and not keys_at:
                keys_at, key_step = len(order), step
            elif entry and item >= 0 and item not in order and item != owner_position:
                order.append(item)
    order.append(owner_position)
    fed_core = 1 - owner_core

    def feed(item, cut):
        lane = pl.multiple_of(tok_at(item, fed_core) * head, head)
        slot = jnp.where(item == owner_position, own_slot, item)
        return remote(
            wq_ref.at[0, depth_of(cut), pl.ds(lane, head)], slots_ref.at[slot, depth_of(cut)],
            feed_sem.at[0, item * CUT + cut], feed_sem.at[1, item * CUT + cut], (twin, col),
        )

    def feed_keys(cut):
        return remote(
            wk_ref.at[0, depth_of(cut), pl.ds(fed_core * head, head)],
            slots_ref.at[key_slot + fed_core, depth_of(cut)],
            feed_sem.at[0, CHIPS * CUT + cut], feed_sem.at[1, CHIPS * CUT + cut], (twin, col),
        )

    def feed_some(first, last):
        loop((last - first) * CUT, lambda at: feed(choose(at // CUT + first, order), at % CUT).start())

    @pl.when(is_owner)
    def _():
        feed_some(0, keys_at)
        loop(CUT, lambda cut: feed_keys(cut).start())
        feed_some(keys_at, CHIPS)

    def through(source, buffer, target, sem):
        take = pltpu.make_async_copy(source, buffer, sem)
        take.start()
        take.wait()
        put = pltpu.make_async_copy(buffer, target, sem)
        put.start()
        put.wait()

    take.wait()
    strip, few = 16, 32

    def normalize_strip(at):
        some = pl.ds(pl.multiple_of(at * strip, strip), strip)
        wide = n_buf[some, :].astype(jnp.float32)
        meansq = jnp.sum(wide * wide, axis=1, keepdims=True) / wide.shape[1]
        n_buf[some, :] = (wide * lax.rsqrt(meansq + 1e-05) * gain_ref[...]).astype(n_buf.dtype)

    loop(block // strip, normalize_strip)

    put = pltpu.make_async_copy(
        n_buf.at[:, pl.ds(pl.multiple_of(col * features, features), features)],
        all_ref.at[pl.ds(pl.multiple_of(tok * block, block), block)], local_sem.at[0],
    )
    put.start()
    keep = pltpu.make_async_copy(n_buf, normed_ref, local_sem.at[2])
    keep.start()

    def clear(at):
        gram[pl.ds(pl.multiple_of(at * few, few), few), :] = jnp.zeros((few, out_cols), jnp.float32)

    put.wait()
    loop(CUT, lambda cut: pass_tokens(position, cut))

    tables = [[packed_table(owner_at, direction, late) for direction in range(3)] for late in (False, True)]
    length = len(tables[0][0][0])
    mine = [
        [
            choose(position, [tables[late][direction][p][i] for p in range(CHIPS)])
            for direction in range(3)
            for i in range(length)
        ]
        for late in range(2)
    ]

    def entry_at(late, direction, step):
        number = choose(direction * length + step // PACK, mine[late])
        return number // choose(step % PACK, [BASE**j for j in range(PACK)]) % BASE

    slots, job_numbers, last_slots = job_table(owner_at)
    last_slot = choose(position, last_slots)
    my_jobs = [choose(position, [job_numbers[p][i] for p in range(CHIPS)]) for i in range(len(job_numbers[0]))]

    def job_at(slot):
        return choose(slot // PACK, my_jobs) // choose(slot % PACK, [BASE**j for j in range(PACK)]) % BASE

    def wait_remote(ref, sem):
        remote(ref, ref, twin_send.at[0], sem, (twin, col)).wait_recv()

    def load_block(item, slot):
        return pltpu.make_async_copy(all_ref.at[chip_rows(item)], g_buf.at[slot % 2], load_sem.at[0, slot % 2])

    def load_columns(source, slot):
        return pltpu.make_async_copy(source, c_buf.at[slot % 2], load_sem.at[1, slot % 2])

    def store_tile(at):
        some = pl.ds(pl.multiple_of(at * out_cols, out_cols), out_cols)
        return pltpu.make_async_copy(gram.at[some], gram_ref.at[some], local_sem.at[3])

    def slot_body(slot):
        item = job_at(slot) - 1

        @pl.when(item >= 0)
        def _():
            wait_remote(all_ref.at[pl.ds(0, block)], twin_recv.at[item])
            load_block(item, slot).start()

            @pl.when(gives_columns)
            def _():
                load_columns(all_ref.at[chip_rows(item), columns_of(tok)], slot).start()

            @pl.when(jnp.logical_not(gives_columns))
            def _():
                for which in range(CORES):
                    wait_remote(cols_ref.at[pl.ds(0, block)], cross_recv.at[which * CHIPS + item])
                load_columns(cols_ref.at[chip_rows(item)], slot).start()

        before = job_at(slot - 1) - 1
        at = (slot + 1) % 2

        @pl.when(before >= 0)
        def _():
            load_block(before, slot - 1).wait()
            load_columns(cols_ref.at[pl.ds(0, rows_in_chip)], slot - 1).wait()
            tile = out_cols

            def term(some):
                lanes = pl.ds(pl.multiple_of(some * tile, tile), tile)
                gram[lanes, :] += lax.dot_general(
                    g_buf[at, :, lanes], c_buf[at], (((0,), (0,)), ((), ())), preferred_element_type=jnp.float32
                )

                @pl.when(final & (some > 0))
                def _():
                    store_tile(some - 1).start()

            final = slot - 1 == last_slot
            loop(features // tile, term)

            @pl.when(final)
            def _():
                store_tile(features // tile - 1).start()

    def arrived(entry):
        item, cut = (entry - 1) // CUT, (entry - 1) % CUT
        rows = rows_of(0, 0)
        remote(all_ref.at[rows], all_ref.at[rows], send_sem.at[0, 0], recv_sem.at[entry - 1], (twin, col)).wait_recv()

        @pl.when(item < CHIPS)
        def _():
            pass_tokens(item, cut)

        @pl.when(item == key_item)
        def _():
            pass_keys(cut)

        @pl.when((item == position + CHIPS) & (item != key_item))
        def _():
            pass_weights(cut)

    def send(source, target, direction, entry, step):
        return remote(
            source, target, send_sem.at[direction, step], recv_sem.at[entry - 1], (choose(direction, neighbour), col)
        )

    def send_tokens(direction, entry, step):
        rows = rows_of((entry - 1) // CUT, (entry - 1) % CUT)
        return send(all_ref.at[rows], all_ref.at[rows], direction, entry, step)

    def send_weights(direction, entry, step, stored):
        item, cut = (entry - 1) // CUT, (entry - 1) % CUT
        target = slots_ref.at[slot_of(item, choose(direction, neighbour_position)), depth_of(cut)]
        lane = pl.multiple_of(tok_at(item - CHIPS, core) * head, head)
        if stored:
            source = wq_ref.at[0, depth_of(cut), pl.ds(lane, head)]
        else:
            source = slots_ref.at[slot_of(item, position), depth_of(cut)]
        return send(source, target, direction, entry, step)

    def fed(at):
        ref = slots_ref.at[own_slot, depth_of(0)]
        remote(ref, ref, feed_sem.at[0, at], feed_sem.at[1, at], (twin, col)).wait_recv()

    head_step = 8

    def step_body(step):
        @pl.when(is_owner & (step == key_step))
        def _():
            source = wk_ref.at[0, :, pl.ds(owner_core * head, head)]
            through(source, w_buf, slots_ref.at[key_slot + owner_core], local_sem.at[1])
            loop(CUT, pass_keys)

        @pl.when(is_owner & (step == head_step))
        def _():
            source = wq_ref.at[0, :, pl.ds(owner * head, head)]
            through(source, w_buf, slots_ref.at[own_slot], local_sem.at[1])
            loop(CUT, pass_weights)

        @pl.when(is_fed & (step == key_step))
        def _():
            def take(cut):
                fed(CHIPS * CUT + cut)
                pass_keys(cut)

            loop(CUT, take)

        @pl.when(is_fed & (step == head_step))
        def _():
            def take(cut):
                fed(owner_position * CUT + cut)
                pass_weights(cut)

            loop(CUT, take)

        def receive(direction):
            entry = entry_at(1, direction, step)

            @pl.when(entry > 0)
            def _():
                arrived(entry)

        loop(3, receive)

        def forward(direction):
            entry = entry_at(0, direction, step)
            item = (entry - 1) // CUT
            stored = is_owner & (item != key_item)

            @pl.when((entry > 0) & (item < CHIPS))
            def _():
                send_tokens(direction, entry, step).start()

            @pl.when((item >= CHIPS) & is_fed & (item != key_item))
            def _():
                fed(entry - 1 - CHIPS * CUT)

            @pl.when((item >= CHIPS) & stored)
            def _():
                send_weights(direction, entry, step, True).start()

            @pl.when((item >= CHIPS) & jnp.logical_not(stored))
            def _():
                send_weights(direction, entry, step, False).start()

        loop(3, forward)

        @pl.when(step == 0)
        def _():
            loop(features // few, clear)

        loop(SLOTS * step + SLOTS, slot_body, SLOTS * step)

    steps = length * PACK
    loop(steps, step_body)
    loop(max(slots + 1, SLOTS * steps), slot_body, SLOTS * steps)

    def drain(at):
        step, direction = at // 3, at % 3

        @pl.when(entry_at(0, direction, step) > 0)
        def _():
            send_tokens(direction, jnp.int32(1), step).wait_send()

    loop(3 * steps, drain)

    @pl.when(is_owner)
    def _():
        loop(CHIPS * CUT, lambda at: feed(at // CUT, at % CUT).wait_send())
        loop(CUT, lambda cut: feed_keys(cut).wait_send())

    halves = all_ref.at[pl.ds(0, all_ref.shape[0] // CORES)]
    remote(halves, halves, twin_send.at[0], twin_recv.at[0], (twin, col)).wait_send()
    keys = slots_ref.at[key_slot]
    remote(keys, keys, twin_send.at[1], twin_recv.at[CHIPS], (twin, col)).wait()
    remote(other_ref, other_ref, cross_send.at[1], cross_recv.at[CORES * CHIPS], (tok, partner)).wait()

    @pl.when(gives_columns)
    def _():
        remote(cols_ref, cols_ref, cross_send.at[0], cross_recv.at[0], (tok, partner)).wait_send()

    keep.wait()
    pltpu.make_async_copy(gram, gram_ref, local_sem.at[3]).wait()


def exchange(owner, hidden, gain, wq, wk):
    block, width = hidden.shape
    groups = CHIPS * CORES
    features = width // lax.axis_size("col")
    depth = wq.shape[1]
    head = wk.shape[2] // CORES
    out_cols = width // groups
    rows = CORES * block
    steps = max(send_steps(owner_at) for owner_at in range(len(ROUTES)))
    kind, wide = hidden.dtype, jnp.float32
    any_space = pl.BlockSpec(memory_space=pl.ANY)
    vmem = pl.BlockSpec(memory_space=pltpu.VMEM)
    gathered, _, slots, other, normed, gram = pl.pallas_call(
        functools.partial(exchange_kernel, owner),
        out_shape=(
            jax.ShapeDtypeStruct((groups * block, features), kind),
            jax.ShapeDtypeStruct((groups * block, out_cols), kind),
            jax.ShapeDtypeStruct((CHIPS + 3, depth, head), kind),
            jax.ShapeDtypeStruct((depth // 2, head), kind),
            jax.ShapeDtypeStruct((block, width), kind),
            jax.ShapeDtypeStruct((features, out_cols), wide),
        ),
        in_specs=[any_space, vmem, any_space, any_space],
        out_specs=(any_space,) * 6,
        scratch_shapes=[
            pltpu.VMEM((block, width), kind),
            pltpu.VMEM((depth, head), kind),
            pltpu.VMEM((features, out_cols), wide),
            pltpu.VMEM((2, rows, features), kind),
            pltpu.VMEM((2, rows, out_cols), kind),
            pltpu.SemaphoreType.DMA((4,)),
            pltpu.SemaphoreType.DMA((2 * CHIPS * CUT,)),
            pltpu.SemaphoreType.DMA((3, steps)),
            pltpu.SemaphoreType.DMA((2, (CHIPS + 1) * CUT)),
            pltpu.SemaphoreType.DMA((2,)),
            pltpu.SemaphoreType.DMA((CHIPS + 1,)),
            pltpu.SemaphoreType.DMA((2,)),
            pltpu.SemaphoreType.DMA((CORES * CHIPS + 1,)),
            pltpu.SemaphoreType.DMA((2, 2)),
        ],
        compiler_params=pltpu.CompilerParams(collective_id=owner, has_side_effects=True),
    )(hidden, gain, wq, wk)
    return gathered, slots, other, normed, gram


def finish_kernel(
    all_ref, slots_ref, other_ref, normed_ref, cos_ref, sin_ref, q_ref, k_ref,
    w_buf, g_buf, n_buf, kw_buf, acc, own_buf, part_buf, part_recv, sum_buf, heads,
    load_sem, w_sem, part_sem, sum_sem, head_sem, keep_sem,
):
    tok, col = lax.axis_index("tok"), lax.axis_index("col")
    groups = CHIPS * CORES
    chip, partner = tok // CORES, 1 - col
    features, head = other_ref.shape
    rows = all_ref.shape[0] // CHIPS
    block = rows // CORES
    depth = slots_ref.shape[1]
    key_slot = CHIPS + 1

    def loop(count, body, first=0):
        def step(at, carry):
            body(at)
            return carry

        lax.fori_loop(first, count, step, 0)

    barrier = pltpu.get_barrier_semaphore()

    def greet(at):
        pl.semaphore_signal(barrier, inc=1, device_id=(lax.rem(tok + at, groups), col), device_id_type=MESH)

    loop(groups, greet, 1)
    pl.semaphore_signal(barrier, inc=1, device_id=(tok, partner), device_id_type=MESH)

    def load(at):
        where = lax.rem(chip + 1 + at, CHIPS)
        return pltpu.make_async_copy(
            all_ref.at[pl.ds(pl.multiple_of(where * rows, rows), rows)], g_buf.at[at % 2], load_sem.at[at % 2]
        )

    own = pltpu.make_async_copy(
        slots_ref.at[CHIPS, pl.ds(pl.multiple_of(col * features, features), features)],
        w_buf.at[:, pl.ds(0, head)], w_sem.at[0],
    )
    own.start()
    crossed = pltpu.make_async_copy(other_ref, w_buf.at[:, pl.ds(head, head)], w_sem.at[1])
    crossed.start()
    load(0).start()
    later = [pltpu.make_async_copy(normed_ref, n_buf, w_sem.at[2])]
    for which in range(CORES):
        later.append(
            pltpu.make_async_copy(
                slots_ref.at[key_slot + which], kw_buf.at[:, pl.ds(which * head, head)], w_sem.at[3 + which]
            )
        )
    own.wait()
    crossed.wait()

    def cross(at):
        return pltpu.make_async_remote_copy(
            src_ref=part_buf.at[at], dst_ref=part_recv.at[at], send_sem=part_sem.at[0, at], recv_sem=part_sem.at[1, at],
            device_id=(tok, partner), device_id_type=MESH,
        )

    def hand(at, which):
        source = sum_buf.at[at, pl.ds(which * block, block)]
        target = lax.rem(chip + 1 + at, CHIPS) * CORES + which
        away = pltpu.make_async_remote_copy(
            src_ref=source, dst_ref=heads.at[tok], send_sem=sum_sem.at[at, which], recv_sem=head_sem.at[0],
            device_id=(target, col), device_id_type=MESH,
        )
        return target, away, pltpu.make_async_copy(source, heads.at[tok], keep_sem.at[0])

    even = lax.broadcasted_iota(jnp.int32, (block, head), 1) % 2 == 0

    def turned(raw):
        swapped = jnp.where(even, pltpu.roll(raw, head - 1, 1), pltpu.roll(raw, 1, 1))
        return raw * cos_ref[...] + swapped * sin_ref[...]

    tile = Q_TILE
    def query(at):
        acc[...] = jnp.zeros(acc.shape, jnp.float32)

        def term(some):
            lanes = pl.ds(pl.multiple_of(some * tile, tile), tile)
            acc[...] += jnp.dot(g_buf[at % 2, :, lanes], w_buf[lanes, :], preferred_element_type=jnp.float32)

        loop(features // tile, term)
        own_buf[at] = acc[:, :head]
        part_buf[at] = acc[:, head:].astype(part_buf.dtype)

    def key():
        some_acc = acc.at[pl.ds(0, block)]
        some_acc[...] = jnp.zeros(some_acc.shape, jnp.float32)

        def term(some):
            lanes = pl.ds(pl.multiple_of(some * tile, tile), tile)
            some_acc[...] += jnp.dot(n_buf[:, lanes], kw_buf[lanes, :], preferred_element_type=jnp.float32)

        loop(depth // tile, term)

        def finish_key(which):
            lanes = pl.ds(pl.multiple_of(which * head, head), head)
            k_ref[:, lanes] = turned(some_acc[:, lanes]).astype(k_ref.dtype)

        loop(CORES, finish_key)

    hand_lag, sum_lag = 3, 2

    def body(at):
        @pl.when(at < CHIPS)
        def _():
            load(at).wait()

        @pl.when(at + 1 < CHIPS)
        def _():
            load(at + 1).start()

        @pl.when(at == 0)
        def _():
            for copy in later:
                copy.start()
            pl.semaphore_wait(barrier, groups)

        @pl.when((at >= 1) & (at < CHIPS + 1))
        def _():
            cross(at - 1).start()

        @pl.when((at >= hand_lag) & (at < CHIPS + hand_lag))
        def _():
            for which in range(CORES):
                target, away, keep = hand(at - hand_lag, which)

                @pl.when(target != tok)
                def _():
                    away.start()

                @pl.when(target == tok)
                def _():
                    keep.start()

        @pl.when(at < CHIPS)
        def _():
            query(at)

        @pl.when(at == CHIPS)
        def _():
            for copy in later:
                copy.wait()
            key()

        @pl.when((at >= sum_lag) & (at < CHIPS + sum_lag))
        def _():
            done = at - sum_lag
            cross(done).wait_recv()
            sum_buf[done] = (own_buf[done] + part_recv[done].astype(jnp.float32)).astype(sum_buf.dtype)

    loop(CHIPS + hand_lag, body)

    def drain(at):
        cross(at).wait_send()
        for which in range(CORES):
            target, away, keep = hand(at, which)

            @pl.when(target != tok)
            def _():
                away.wait_send()

            @pl.when(target == tok)
            def _():
                keep.wait()

    loop(CHIPS, drain)
    others = heads.at[pl.ds(0, groups - 1)]
    pltpu.make_async_remote_copy(
        src_ref=others, dst_ref=others, send_sem=sum_sem.at[0, 0], recv_sem=head_sem.at[0],
        device_id=(tok, partner), device_id_type=MESH,
    ).wait_recv()

    def finish_head(at):
        lanes = pl.ds(pl.multiple_of(at * head, head), head)
        q_ref[:, lanes] = turned(heads[at].astype(jnp.float32)).astype(q_ref.dtype)

    loop(groups, finish_head)


Q_TILE = 1024


def finish(gathered, slots, other, normed, cosine, sine):
    features, head = other.shape
    groups = CHIPS * CORES
    rows = gathered.shape[0] // CHIPS
    block = rows // CORES
    depth = slots.shape[1]
    kind, wide = gathered.dtype, jnp.float32
    any_space = pl.BlockSpec(memory_space=pl.ANY)
    vmem = pl.BlockSpec(memory_space=pltpu.VMEM)
    return pl.pallas_call(
        finish_kernel,
        out_shape=(
            jax.ShapeDtypeStruct((block, groups * head), kind),
            jax.ShapeDtypeStruct((block, CORES * head), kind),
        ),
        in_specs=[any_space] * 4 + [vmem] * 2,
        out_specs=(vmem, vmem),
        scratch_shapes=[
            pltpu.VMEM((features, 2 * head), kind),
            pltpu.VMEM((2, rows, features), kind),
            pltpu.VMEM((block, depth), kind),
            pltpu.VMEM((depth, CORES * head), kind),
            pltpu.VMEM((rows, 2 * head), wide),
            pltpu.VMEM((CHIPS, rows, head), wide),
            pltpu.VMEM((CHIPS, rows, head), kind),
            pltpu.VMEM((CHIPS, rows, head), kind),
            pltpu.VMEM((CHIPS, rows, head), kind),
            pltpu.VMEM((groups, block, head), kind),
            pltpu.SemaphoreType.DMA((2,)),
            pltpu.SemaphoreType.DMA((3 + CORES,)),
            pltpu.SemaphoreType.DMA((2, CHIPS)),
            pltpu.SemaphoreType.DMA((CHIPS, CORES)),
            pltpu.SemaphoreType.DMA((1,)),
            pltpu.SemaphoreType.DMA((1,)),
        ],
        compiler_params=pltpu.CompilerParams(collective_id=groups, has_side_effects=True),
    )(gathered, slots, other, normed, cosine, sine)


def angles(place):
    dims = jnp.arange(HEAD, dtype=jnp.int32)
    pair = (dims // 2).astype(jnp.float32)
    freq = jnp.power(jnp.float32(rope_base), -2.0 * pair / HEAD)
    angle = place.astype(jnp.float32)[:, None] * freq[None, :]
    sine = jnp.where((dims % 2 == 0)[None, :], -jnp.sin(angle), jnp.sin(angle))
    return jnp.cos(angle), sine


def grid_shards(hidden, norm_gain, token_ids, owner, query_store, key_store):
    cosine, sine = lax.optimization_barrier(angles(positions(token_ids)))
    groups = lax.axis_size("tok")
    branches = [functools.partial(exchange, at) for at in range(groups)]
    gathered, slots, other, normed, gram = lax.switch(owner[0], branches, hidden, norm_gain[None, :], query_store, key_store)
    queries, keys = finish(gathered, slots, other, normed, cosine, sine)
    return (queries, keys, gram * (2.0 / (hidden.shape[0] * groups)))


def solution(mesh):
    placed = (P("tok", None), P(), P("tok"), P(), P("tok", None, "col"), P("tok", None, "col"))
    fits = mesh.shape["tok"] == CHIPS * CORES and mesh.shape["col"] == 2
    return jax.shard_map(
        grid_shards if fits else shards,
        mesh=mesh,
        in_specs=placed,
        out_specs=(P("tok", "col"), P("tok", "col"), P("col", "tok")),
        check_vma=False,
    )
```

```python
import functools

import jax
import jax.numpy as jnp
from jax import lax
from jax.experimental import pallas as pl
from jax.experimental.pallas import tpu as pltpu
from jax.sharding import PartitionSpec as P

HEAD = 128
SEQ = 128


begin_token = 128000
rope_base = 500000.0


def scatter_weights(query, key, owner):
    groups = lax.axis_size("tok")
    depth, width = query.shape
    piece = width // groups
    mine = lax.axis_index("tok") == owner
    query = jnp.moveaxis(query.reshape(depth, groups, piece), 1, 0)
    key = key.reshape(groups, depth * key.shape[1] // groups // piece, piece)
    both = jnp.concatenate([query, key], axis=1)
    return jnp.where(mine, both, jnp.zeros_like(both))


def positions(token_ids):
    samples = token_ids.reshape(-1, SEQ)
    index = jnp.arange(SEQ, dtype=jnp.int32)
    starts = jnp.where(samples == begin_token, index[None, :], jnp.zeros_like(samples))
    latest = lax.cummax(starts, axis=1)
    return (index[None, :] - latest).reshape(-1)


def rotate(values, place, start):
    width = values.shape[1]
    period = HEAD if width % HEAD == 0 else width
    dims = (start + jnp.arange(period, dtype=jnp.int32)) % HEAD
    pair = (dims // 2).astype(jnp.float32)
    freq = jnp.power(jnp.float32(rope_base), -2.0 * pair / HEAD)
    angle = place.astype(jnp.float32)[:, None] * freq[None, :]
    even = dims % 2 == 0
    sine = jnp.where(even[None, :], -jnp.sin(angle), jnp.sin(angle))
    cosine, sine = lax.optimization_barrier((jnp.cos(angle), sine))
    cosine = jnp.tile(cosine, (1, width // period))
    sine = jnp.tile(sine, (1, width // period))
    following = jnp.concatenate([values[:, 1:], values[:, :1]], axis=1)
    previous = jnp.concatenate([values[:, -1:], values[:, :-1]], axis=1)
    even = jnp.arange(width, dtype=jnp.int32) % 2 == 0
    other = jnp.where(even[None, :], following, previous)
    return values * cosine + other * sine


def normalize(hidden, norm_gain):
    wide = hidden.astype(jnp.float32)
    meansq = jnp.mean(wide * wide, axis=-1, keepdims=True)
    return (wide * lax.rsqrt(meansq + 1e-05) * norm_gain[None, :]).astype(jnp.bfloat16)


def transposed_product(left, right):
    return lax.dot_general(
        left, right, (((0,), (0,)), ((), ())), preferred_element_type=jnp.float32
    )


def shards(hidden, norm_gain, token_ids, owner, query_store, key_store):
    normed = normalize(hidden, norm_gain)
    place = positions(token_ids)
    column = lax.axis_index("col")
    row_width = normed.shape[1] // lax.axis_size("col")
    row_block = lax.dynamic_slice_in_dim(normed, column * row_width, row_width, 1)
    total_tokens = normed.shape[0] * lax.axis_size("tok")
    groups, parts = lax.axis_size("tok"), lax.axis_size("col")
    depth, q_width = query_store.shape[1:]
    k_width = key_store.shape[2]
    masked = scatter_weights(query_store[0], key_store[0], owner[0])
    gathered = lax.all_gather(row_block, "tok", axis=0, tiled=True)
    col_block = lax.all_to_all(normed, "tok", split_axis=1, concat_axis=0, tiled=True)
    masked, gathered = lax.optimization_barrier((masked, gathered))
    owned = lax.psum_scatter(masked, "tok", scatter_dimension=0, tiled=False)
    gram = transposed_product(gathered, col_block)
    hessian = gram * (2.0 / total_tokens)
    key_rows = owned[depth:].reshape(depth // groups, k_width)
    weight_k = lax.all_gather(key_rows, "tok", axis=0, tiled=True)
    weight_q = lax.all_to_all(owned[:depth], "col", split_axis=0, concat_axis=1, tiled=True)
    partial = jnp.dot(gathered, weight_q, preferred_element_type=jnp.float32).astype(jnp.bfloat16)
    partial = lax.all_to_all(partial, "col", split_axis=1, concat_axis=0, tiled=True)
    partial = partial.reshape(parts, total_tokens, q_width // groups).astype(jnp.float32)
    summed = jnp.sum(partial, axis=0).astype(jnp.bfloat16)
    raw_q = lax.all_to_all(summed, "tok", split_axis=0, concat_axis=1, tiled=True).astype(jnp.float32)
    raw_k = jnp.dot(normed, weight_k, preferred_element_type=jnp.float32)
    queries = rotate(raw_q, place, column * q_width).astype(jnp.bfloat16)
    keys = rotate(raw_k, place, column * k_width).astype(jnp.bfloat16)
    return (queries, keys, hessian)


MESH = pl.DeviceIdType.MESH

DEPTH, WIDE, CORES = 4, 2, 2
CHIPS = DEPTH * WIDE
CUT = 4
LAG = 2
BASE = 128
PACK = 4
ROUTES = (
    (
        (
            (76078909, 8438017, 114118945, 80303143, 25347337),
            (29573893, 42255367, 4127, 0, 0),
            (38028553, 25349401, 97213495, 6191, 0),
            (29575183, 76071685, 8438017, 16896031, 0),
            (38029843, 25354303, 76074265, 8438017, 0),
            (29575957, 21122071, 33800965, 71843840, 1031),
            (38030875, 29575957, 3353, 4215331, 25346563),
            (67620637, 21121555, 3095, 33800965, 16896289),
        ),
        (
            (126804031, 118349113, 101439277, 109893937, 88757803),
            (131023621, 4215331, 71844355, 114115591, 0),
            (135251467, 122576443, 4215331, 105660931, 6707),
            (21120781, 12672829, 118343695, 16896289, 6965),
            (46483729, 126797581, 76078393, 8438017, 1547),
            (42257431, 135251209, 12672829, 71845903, 1031),
            (0, 0, 0, 0, 0),
            (0, 0, 0, 0, 0),
        ),
        (
            (0, 0, 0, 0, 0),
            (0, 0, 0, 0, 0),
            (25347337, 46483729, 63393307, 33803287, 3353),
            (46483213, 67619347, 63393307, 38030359, 54937615),
            (54937873, 59165461, 50712349, 2579, 4385),
            (42257173, 59166751, 50712349, 0, 0),
            (59165977, 67620637, 0, 0, 0),
            (59166751, 3869, 0, 0, 0),
        ),
    ),
    (
        (
            (88752385, 8443435, 21121555, 25349143, 3353),
            (29573893, 46483471, 63393307, 16894225, 4127),
            (84533053, 118346533, 101439277, 25347337, 0),
            (50710285, 16893967, 12668701, 4127, 0),
            (135252241, 42254851, 21122329, 114116107, 0),
            (29575957, 4211719, 92982295, 33800965, 0),
            (42257947, 29575441, 4211977, 54937099, 1031),
            (67620637, 50711317, 88752643, 12670507, 2063),
        ),
        (
            (4211203, 0, 0, 0, 0),
            (4211719, 92984617, 8438533, 0, 0),
            (8446015, 25347337, 122576443, 105667381, 6707),
            (16893709, 88752385, 12670507, 131024911, 7223),
            (38029843, 21120781, 25346305, 126796807, 7481),
            (50711317, 8446015, 92984617, 33800965, 7997),
            (0, 0, 0, 0, 0),
            (0, 0, 0, 0, 0),
        ),
        (
            (0, 0, 0, 0, 0),
            (0, 0, 0, 0, 0),
            (92984617, 21121555, 25349143, 76074265, 4385),
            (33801997, 59165461, 38031133, 84529183, 4901),
            (54938131, 59165461, 2321, 0, 0),
            (46484503, 63393307, 67619089, 54938131, 0),
            (59165977, 67620637, 0, 5417, 0),
            (59166493, 4127, 0, 0, 0),
        ),
    ),
)


def step_entries(owner_at, direction, position):
    entries = []
    for number in ROUTES[owner_at][direction][position]:
        for _ in range(PACK):
            entries.append(number % BASE)
            number //= BASE
    return entries


def packed_table(owner_at, direction, arrivals):
    table = []
    for position in range(CHIPS):
        entries = None
        if not arrivals:
            entries = step_entries(owner_at, direction, position) + [0] * LAG
        else:
            z = position // WIDE + (0, -1, 1)[direction]
            sender = position ^ 1 if direction == 0 else z * WIDE + position % WIDE
            entries = [0] * LAG + (
                step_entries(owner_at, direction, sender) if 0 <= z < DEPTH else [0] * len(step_entries(owner_at, 0, 0))
            )
        entries += [0] * (-len(entries) % PACK)
        table.append([
            sum(entries[i + j] * BASE**j for j in range(PACK)) for i in range(0, len(entries), PACK)
        ])
    return table


def choose(index, options):
    value = jnp.int32(0)
    for at, option in enumerate(options):
        if isinstance(option, int) and option == 0:
            continue
        value = jnp.where(index == at, jnp.int32(option) if isinstance(option, int) else option, value)
    return value


def arrival_steps(owner_at):
    steps = [[None] * (2 * CHIPS) for _ in range(CHIPS)]
    for position in range(CHIPS):
        for direction in range(3):
            z = position // WIDE + (0, 1, -1)[direction]
            target = position ^ 1 if direction == 0 else z * WIDE + position % WIDE
            for step, entry in enumerate(step_entries(owner_at, direction, position)):
                if entry:
                    item = (entry - 1) // CUT
                    steps[target][item] = max(steps[target][item] or 0, step + LAG)
    return steps


SLOTS = 2


def send_steps(owner_at):
    return (len(step_entries(owner_at, 0, 0)) + LAG + PACK - 1) // PACK * PACK


def job_table(owner_at):
    table = []
    for position, steps in enumerate(arrival_steps(owner_at)):
        ready = [1 if item == position else steps[item] + 1 for item in range(CHIPS)]
        waiting = sorted(range(CHIPS), key=lambda item: (ready[item], item))
        jobs = []
        while waiting:
            step = len(jobs) // SLOTS
            jobs.append(waiting.pop(0) + 1 if ready[waiting[0]] <= step else 0)
        table.append(jobs)
    slots = max(len(jobs) for jobs in table)
    packed = []
    for jobs in table:
        jobs = jobs + [0] * (-slots % PACK + slots - len(jobs))
        packed.append([sum(jobs[i + j] * BASE**j for j in range(PACK)) for i in range(0, len(jobs), PACK)])
    return slots, packed, [len(jobs) - 1 for jobs in table]


def exchange_kernel(
    owner, hidden_ref, gain_ref, wq_ref, wk_ref, all_ref, cols_ref, slots_ref, other_ref, normed_ref, gram_ref,
    n_buf, w_buf, gram, g_buf, c_buf,
    local_sem, recv_sem, send_sem, feed_sem, twin_send, twin_recv, cross_send, cross_recv, load_sem,
):
    tok, col = lax.axis_index("tok"), lax.axis_index("col")
    z, y, core = tok // (WIDE * CORES), tok // CORES % WIDE, tok % CORES
    owner_z, owner_y, owner_core = owner // (WIDE * CORES), owner // CORES % WIDE, owner % CORES
    flip = owner_z >= DEPTH // 2
    owner_at = DEPTH - 1 - owner_z if flip else owner_z
    owner_position = owner_at * WIDE
    key_item = CHIPS + owner_position
    near_z = DEPTH - 1 - z if flip else z
    position = near_z * WIDE + (y + owner_y) % WIDE
    block, features = hidden_ref.shape[0], all_ref.shape[1]
    rows_in_chip = CORES * block
    piece = block // CUT
    head = slots_ref.shape[2]
    depth = slots_ref.shape[1]
    part = depth // CUT
    out_cols = cols_ref.shape[1]
    own_slot, key_slot = CHIPS, CHIPS + 1
    at_owner = position == owner_position
    is_owner = at_owner & (core == owner_core)
    is_fed = at_owner & (core != owner_core)

    def chip_at(where):
        at_z = where // WIDE
        at_z = DEPTH - 1 - at_z if flip else at_z
        return at_z * WIDE + (where % WIDE + owner_y) % WIDE

    def tok_at(where, which):
        return chip_at(where) * CORES + which

    up, down = (tok - WIDE * CORES, tok + WIDE * CORES) if flip else (tok + WIDE * CORES, tok - WIDE * CORES)
    beside = tok + CORES - 2 * CORES * y
    twin = tok + 1 - 2 * core
    partner = 1 - col
    neighbour = (beside, up, down)
    neighbour_position = (position + 1 - 2 * (position % WIDE), position + WIDE, position - WIDE)
    present = (y >= 0, near_z < DEPTH - 1, near_z > 0)

    barrier = pltpu.get_barrier_semaphore()
    for at, there in zip(neighbour, present):
        @pl.when(there)
        def _():
            pl.semaphore_signal(barrier, inc=1, device_id=(at, col), device_id_type=MESH)
    pl.semaphore_signal(barrier, inc=1, device_id=(twin, col), device_id_type=MESH)
    pl.semaphore_signal(barrier, inc=1, device_id=(tok, partner), device_id_type=MESH)
    pl.semaphore_signal(barrier, inc=1, device_id=(twin, partner), device_id_type=MESH)
    take = pltpu.make_async_copy(hidden_ref, n_buf, local_sem.at[0])
    take.start()
    pl.semaphore_wait(barrier, 4 + jnp.minimum(near_z, 1) + jnp.minimum(DEPTH - 1 - near_z, 1))

    def remote(source, target, sent, received, at):
        return pltpu.make_async_remote_copy(
            src_ref=source, dst_ref=target, send_sem=sent, recv_sem=received, device_id=at, device_id_type=MESH
        )

    def rows_of(item, cut):
        return pl.ds(pl.multiple_of(tok_at(item, core) * block + cut * piece, piece), piece)

    def chip_rows(item):
        return pl.ds(pl.multiple_of(chip_at(item) * rows_in_chip, rows_in_chip), rows_in_chip)

    def depth_of(cut):
        return pl.ds(pl.multiple_of(cut * part, part), part)

    def slot_of(item, at):
        where = item - CHIPS
        return jnp.where(item == key_item, key_slot + core, jnp.where(where == at, own_slot, where))

    gives_columns = z // (DEPTH // 2) == col

    def loop(count, body, first=0):
        def step(at, carry):
            body(at)
            return carry

        lax.fori_loop(first, count, step, 0)

    def columns_of(target):
        return pl.ds(pl.multiple_of(target * out_cols % features, out_cols), out_cols)

    def pass_tokens(item, cut):
        rows = rows_of(item, cut)
        remote(all_ref.at[rows], all_ref.at[rows], twin_send.at[0], twin_recv.at[item], (twin, col)).start()

        @pl.when(gives_columns)
        def _():
            def give(which):
                target = tok - core + which
                remote(
                    all_ref.at[rows, columns_of(target)], cols_ref.at[rows], cross_send.at[0],
                    cross_recv.at[core * CHIPS + item], (target, partner),
                ).start()

            loop(CORES, give)

    def pass_keys(cut):
        ref = slots_ref.at[key_slot + core, depth_of(cut)]
        remote(ref, ref, twin_send.at[1], twin_recv.at[CHIPS], (twin, col)).start()

    def pass_weights(cut):
        @pl.when(cut // (CUT // 2) == partner)
        def _():
            remote(
                slots_ref.at[own_slot, depth_of(cut)],
                other_ref.at[pl.ds(pl.multiple_of(cut % (CUT // 2) * part, part), part)],
                cross_send.at[1], cross_recv.at[CORES * CHIPS], (tok, partner),
            ).start()

    order, keys_at, key_step = [], 0, 0
    for step in range(len(step_entries(owner_at, 0, 0))):
        for direction in (1, 0, 2):
            entry = step_entries(owner_at, direction, owner_position)[step]
            item = (entry - 1) // CUT - CHIPS
            if item == owner_position and not keys_at:
                keys_at, key_step = len(order), step
            elif entry and item >= 0 and item not in order and item != owner_position:
                order.append(item)
    order.append(owner_position)
    fed_core = 1 - owner_core

    def feed(item, cut):
        lane = pl.multiple_of(tok_at(item, fed_core) * head, head)
        slot = jnp.where(item == owner_position, own_slot, item)
        return remote(
            wq_ref.at[0, depth_of(cut), pl.ds(lane, head)], slots_ref.at[slot, depth_of(cut)],
            feed_sem.at[0, item * CUT + cut], feed_sem.at[1, item * CUT + cut], (twin, col),
        )

    def feed_keys(cut):
        return remote(
            wk_ref.at[0, depth_of(cut), pl.ds(fed_core * head, head)],
            slots_ref.at[key_slot + fed_core, depth_of(cut)],
            feed_sem.at[0, CHIPS * CUT + cut], feed_sem.at[1, CHIPS * CUT + cut], (twin, col),
        )

    def feed_some(first, last):
        loop((last - first) * CUT, lambda at: feed(choose(at // CUT + first, order), at % CUT).start())

    @pl.when(is_owner)
    def _():
        feed_some(0, keys_at)
        loop(CUT, lambda cut: feed_keys(cut).start())
        feed_some(keys_at, CHIPS)

    def through(source, buffer, target, sem):
        take = pltpu.make_async_copy(source, buffer, sem)
        take.start()
        take.wait()
        put = pltpu.make_async_copy(buffer, target, sem)
        put.start()
        put.wait()

    take.wait()
    strip, few = 16, 32

    def normalize_strip(at):
        some = pl.ds(pl.multiple_of(at * strip, strip), strip)
        wide = n_buf[some, :].astype(jnp.float32)
        meansq = jnp.sum(wide * wide, axis=1, keepdims=True) / wide.shape[1]
        n_buf[some, :] = (wide * lax.rsqrt(meansq + 1e-05) * gain_ref[...]).astype(n_buf.dtype)

    loop(block // strip, normalize_strip)

    put = pltpu.make_async_copy(
        n_buf.at[:, pl.ds(pl.multiple_of(col * features, features), features)],
        all_ref.at[pl.ds(pl.multiple_of(tok * block, block), block)], local_sem.at[0],
    )
    put.start()
    keep = pltpu.make_async_copy(n_buf, normed_ref, local_sem.at[2])
    keep.start()

    def clear(at):
        gram[pl.ds(pl.multiple_of(at * few, few), few), :] = jnp.zeros((few, out_cols), jnp.float32)

    put.wait()
    loop(CUT, lambda cut: pass_tokens(position, cut))

    tables = [[packed_table(owner_at, direction, late) for direction in range(3)] for late in (False, True)]
    length = len(tables[0][0][0])
    mine = [
        [
            choose(position, [tables[late][direction][p][i] for p in range(CHIPS)])
            for direction in range(3)
            for i in range(length)
        ]
        for late in range(2)
    ]

    def entry_at(late, direction, step):
        number = choose(direction * length + step // PACK, mine[late])
        return number // choose(step % PACK, [BASE**j for j in range(PACK)]) % BASE

    slots, job_numbers, last_slots = job_table(owner_at)
    last_slot = choose(position, last_slots)
    my_jobs = [choose(position, [job_numbers[p][i] for p in range(CHIPS)]) for i in range(len(job_numbers[0]))]

    def job_at(slot):
        return choose(slot // PACK, my_jobs) // choose(slot % PACK, [BASE**j for j in range(PACK)]) % BASE

    def wait_remote(ref, sem):
        remote(ref, ref, twin_send.at[0], sem, (twin, col)).wait_recv()

    def load_block(item, slot):
        return pltpu.make_async_copy(all_ref.at[chip_rows(item)], g_buf.at[slot % 2], load_sem.at[0, slot % 2])

    def load_columns(source, slot):
        return pltpu.make_async_copy(source, c_buf.at[slot % 2], load_sem.at[1, slot % 2])

    def store_tile(at):
        some = pl.ds(pl.multiple_of(at * out_cols, out_cols), out_cols)
        return pltpu.make_async_copy(gram.at[some], gram_ref.at[some], local_sem.at[3])

    def slot_body(slot):
        item = job_at(slot) - 1

        @pl.when(item >= 0)
        def _():
            wait_remote(all_ref.at[pl.ds(0, block)], twin_recv.at[item])
            load_block(item, slot).start()

            @pl.when(gives_columns)
            def _():
                load_columns(all_ref.at[chip_rows(item), columns_of(tok)], slot).start()

            @pl.when(jnp.logical_not(gives_columns))
            def _():
                for which in range(CORES):
                    wait_remote(cols_ref.at[pl.ds(0, block)], cross_recv.at[which * CHIPS + item])
                load_columns(cols_ref.at[chip_rows(item)], slot).start()

        before = job_at(slot - 1) - 1
        at = (slot + 1) % 2

        @pl.when(before >= 0)
        def _():
            load_block(before, slot - 1).wait()
            load_columns(cols_ref.at[pl.ds(0, rows_in_chip)], slot - 1).wait()
            tile = out_cols

            def term(some):
                lanes = pl.ds(pl.multiple_of(some * tile, tile), tile)
                gram[lanes, :] += lax.dot_general(
                    g_buf[at, :, lanes], c_buf[at], (((0,), (0,)), ((), ())), preferred_element_type=jnp.float32
                )

                @pl.when(final & (some > 0))
                def _():
                    store_tile(some - 1).start()

            final = slot - 1 == last_slot
            loop(features // tile, term)

            @pl.when(final)
            def _():
                store_tile(features // tile - 1).start()

    def arrived(entry):
        item, cut = (entry - 1) // CUT, (entry - 1) % CUT
        rows = rows_of(0, 0)
        remote(all_ref.at[rows], all_ref.at[rows], send_sem.at[0, 0], recv_sem.at[entry - 1], (twin, col)).wait_recv()

        @pl.when(item < CHIPS)
        def _():
            pass_tokens(item, cut)

        @pl.when(item == key_item)
        def _():
            pass_keys(cut)

        @pl.when((item == position + CHIPS) & (item != key_item))
        def _():
            pass_weights(cut)

    def send(source, target, direction, entry, step):
        return remote(
            source, target, send_sem.at[direction, step], recv_sem.at[entry - 1], (choose(direction, neighbour), col)
        )

    def send_tokens(direction, entry, step):
        rows = rows_of((entry - 1) // CUT, (entry - 1) % CUT)
        return send(all_ref.at[rows], all_ref.at[rows], direction, entry, step)

    def send_weights(direction, entry, step, stored):
        item, cut = (entry - 1) // CUT, (entry - 1) % CUT
        target = slots_ref.at[slot_of(item, choose(direction, neighbour_position)), depth_of(cut)]
        lane = pl.multiple_of(tok_at(item - CHIPS, core) * head, head)
        if stored:
            source = wq_ref.at[0, depth_of(cut), pl.ds(lane, head)]
        else:
            source = slots_ref.at[slot_of(item, position), depth_of(cut)]
        return send(source, target, direction, entry, step)

    def fed(at):
        ref = slots_ref.at[own_slot, depth_of(0)]
        remote(ref, ref, feed_sem.at[0, at], feed_sem.at[1, at], (twin, col)).wait_recv()

    head_step = 8

    def step_body(step):
        @pl.when(is_owner & (step == key_step))
        def _():
            source = wk_ref.at[0, :, pl.ds(owner_core * head, head)]
            through(source, w_buf, slots_ref.at[key_slot + owner_core], local_sem.at[1])
            loop(CUT, pass_keys)

        @pl.when(is_owner & (step == head_step))
        def _():
            source = wq_ref.at[0, :, pl.ds(owner * head, head)]
            through(source, w_buf, slots_ref.at[own_slot], local_sem.at[1])
            loop(CUT, pass_weights)

        @pl.when(is_fed & (step == key_step))
        def _():
            def take(cut):
                fed(CHIPS * CUT + cut)
                pass_keys(cut)

            loop(CUT, take)

        @pl.when(is_fed & (step == head_step))
        def _():
            def take(cut):
                fed(owner_position * CUT + cut)
                pass_weights(cut)

            loop(CUT, take)

        def receive(direction):
            entry = entry_at(1, direction, step)

            @pl.when(entry > 0)
            def _():
                arrived(entry)

        loop(3, receive)

        def forward(direction):
            entry = entry_at(0, direction, step)
            item = (entry - 1) // CUT
            stored = is_owner & (item != key_item)

            @pl.when((entry > 0) & (item < CHIPS))
            def _():
                send_tokens(direction, entry, step).start()

            @pl.when((item >= CHIPS) & is_fed & (item != key_item))
            def _():
                fed(entry - 1 - CHIPS * CUT)

            @pl.when((item >= CHIPS) & stored)
            def _():
                send_weights(direction, entry, step, True).start()

            @pl.when((item >= CHIPS) & jnp.logical_not(stored))
            def _():
                send_weights(direction, entry, step, False).start()

        loop(3, forward)

        @pl.when(step == 0)
        def _():
            loop(features // few, clear)

        loop(SLOTS * step + SLOTS, slot_body, SLOTS * step)

    steps = length * PACK
    loop(steps, step_body)
    loop(max(slots + 1, SLOTS * steps), slot_body, SLOTS * steps)

    def drain(at):
        step, direction = at // 3, at % 3

        @pl.when(entry_at(0, direction, step) > 0)
        def _():
            send_tokens(direction, jnp.int32(1), step).wait_send()

    loop(3 * steps, drain)

    @pl.when(is_owner)
    def _():
        loop(CHIPS * CUT, lambda at: feed(at // CUT, at % CUT).wait_send())
        loop(CUT, lambda cut: feed_keys(cut).wait_send())

    halves = all_ref.at[pl.ds(0, all_ref.shape[0] // CORES)]
    remote(halves, halves, twin_send.at[0], twin_recv.at[0], (twin, col)).wait_send()
    keys = slots_ref.at[key_slot]
    remote(keys, keys, twin_send.at[1], twin_recv.at[CHIPS], (twin, col)).wait()
    remote(other_ref, other_ref, cross_send.at[1], cross_recv.at[CORES * CHIPS], (tok, partner)).wait()

    @pl.when(gives_columns)
    def _():
        remote(cols_ref, cols_ref, cross_send.at[0], cross_recv.at[0], (tok, partner)).wait_send()

    keep.wait()
    pltpu.make_async_copy(gram, gram_ref, local_sem.at[3]).wait()


def exchange(owner, hidden, gain, wq, wk):
    block, width = hidden.shape
    groups = CHIPS * CORES
    features = width // lax.axis_size("col")
    depth = wq.shape[1]
    head = wk.shape[2] // CORES
    out_cols = width // groups
    rows = CORES * block
    steps = max(send_steps(owner_at) for owner_at in range(len(ROUTES)))
    kind, wide = hidden.dtype, jnp.float32
    any_space = pl.BlockSpec(memory_space=pl.ANY)
    vmem = pl.BlockSpec(memory_space=pltpu.VMEM)
    gathered, _, slots, other, normed, gram = pl.pallas_call(
        functools.partial(exchange_kernel, owner),
        out_shape=(
            jax.ShapeDtypeStruct((groups * block, features), kind),
            jax.ShapeDtypeStruct((groups * block, out_cols), kind),
            jax.ShapeDtypeStruct((CHIPS + 3, depth, head), kind),
            jax.ShapeDtypeStruct((depth // 2, head), kind),
            jax.ShapeDtypeStruct((block, width), kind),
            jax.ShapeDtypeStruct((features, out_cols), wide),
        ),
        in_specs=[any_space, vmem, any_space, any_space],
        out_specs=(any_space,) * 6,
        scratch_shapes=[
            pltpu.VMEM((block, width), kind),
            pltpu.VMEM((depth, head), kind),
            pltpu.VMEM((features, out_cols), wide),
            pltpu.VMEM((2, rows, features), kind),
            pltpu.VMEM((2, rows, out_cols), kind),
            pltpu.SemaphoreType.DMA((4,)),
            pltpu.SemaphoreType.DMA((2 * CHIPS * CUT,)),
            pltpu.SemaphoreType.DMA((3, steps)),
            pltpu.SemaphoreType.DMA((2, (CHIPS + 1) * CUT)),
            pltpu.SemaphoreType.DMA((2,)),
            pltpu.SemaphoreType.DMA((CHIPS + 1,)),
            pltpu.SemaphoreType.DMA((2,)),
            pltpu.SemaphoreType.DMA((CORES * CHIPS + 1,)),
            pltpu.SemaphoreType.DMA((2, 2)),
        ],
        compiler_params=pltpu.CompilerParams(collective_id=owner, has_side_effects=True),
    )(hidden, gain, wq, wk)
    return gathered, slots, other, normed, gram


def finish_kernel(
    all_ref, slots_ref, other_ref, normed_ref, heads, k_ref,
    w_buf, g_buf, n_buf, kw_buf, acc, own_buf, part_buf, part_recv, sum_buf,
    load_sem, w_sem, part_sem, sum_sem, head_sem, keep_sem,
):
    tok, col = lax.axis_index("tok"), lax.axis_index("col")
    groups = CHIPS * CORES
    chip, partner = tok // CORES, 1 - col
    features, head = other_ref.shape
    rows = all_ref.shape[0] // CHIPS
    block = rows // CORES
    depth = slots_ref.shape[1]
    key_slot = CHIPS + 1

    def loop(count, body, first=0):
        def step(at, carry):
            body(at)
            return carry

        lax.fori_loop(first, count, step, 0)

    barrier = pltpu.get_barrier_semaphore()

    def greet(at):
        pl.semaphore_signal(barrier, inc=1, device_id=(lax.rem(tok + at, groups), col), device_id_type=MESH)

    loop(groups, greet, 1)
    pl.semaphore_signal(barrier, inc=1, device_id=(tok, partner), device_id_type=MESH)

    def load(at):
        where = lax.rem(chip + 1 + at, CHIPS)
        return pltpu.make_async_copy(
            all_ref.at[pl.ds(pl.multiple_of(where * rows, rows), rows)], g_buf.at[at % 2], load_sem.at[at % 2]
        )

    own = pltpu.make_async_copy(
        slots_ref.at[CHIPS, pl.ds(pl.multiple_of(col * features, features), features)],
        w_buf.at[:, pl.ds(0, head)], w_sem.at[0],
    )
    own.start()
    crossed = pltpu.make_async_copy(other_ref, w_buf.at[:, pl.ds(head, head)], w_sem.at[1])
    crossed.start()
    load(0).start()
    later = [pltpu.make_async_copy(normed_ref, n_buf, w_sem.at[2])]
    for which in range(CORES):
        later.append(
            pltpu.make_async_copy(
                slots_ref.at[key_slot + which], kw_buf.at[:, pl.ds(which * head, head)], w_sem.at[3 + which]
            )
        )
    own.wait()
    crossed.wait()

    def cross(at):
        return pltpu.make_async_remote_copy(
            src_ref=part_buf.at[at], dst_ref=part_recv.at[at], send_sem=part_sem.at[0, at], recv_sem=part_sem.at[1, at],
            device_id=(tok, partner), device_id_type=MESH,
        )

    def hand(at, which):
        source = sum_buf.at[at, pl.ds(which * block, block)]
        target = lax.rem(chip + 1 + at, CHIPS) * CORES + which
        away = pltpu.make_async_remote_copy(
            src_ref=source, dst_ref=heads.at[tok], send_sem=sum_sem.at[at, which], recv_sem=head_sem.at[0],
            device_id=(target, col), device_id_type=MESH,
        )
        return target, away, pltpu.make_async_copy(source, heads.at[tok], keep_sem.at[0])

    tile = Q_TILE
    def query(at):
        acc[...] = jnp.zeros(acc.shape, jnp.float32)

        def term(some):
            lanes = pl.ds(pl.multiple_of(some * tile, tile), tile)
            acc[...] += jnp.dot(g_buf[at % 2, :, lanes], w_buf[lanes, :], preferred_element_type=jnp.float32)

        loop(features // tile, term)
        own_buf[at] = acc[:, :head]
        part_buf[at] = acc[:, head:].astype(part_buf.dtype)

    def key():
        some_acc = acc.at[pl.ds(0, block)]
        some_acc[...] = jnp.zeros(some_acc.shape, jnp.float32)

        def term(some):
            lanes = pl.ds(pl.multiple_of(some * tile, tile), tile)
            some_acc[...] += jnp.dot(n_buf[:, lanes], kw_buf[lanes, :], preferred_element_type=jnp.float32)

        loop(depth // tile, term)

        k_ref[...] = some_acc[...]

    hand_lag, sum_lag = 3, 2

    def body(at):
        @pl.when(at < CHIPS)
        def _():
            load(at).wait()

        @pl.when(at + 1 < CHIPS)
        def _():
            load(at + 1).start()

        @pl.when(at == 0)
        def _():
            for copy in later:
                copy.start()
            pl.semaphore_wait(barrier, groups)

        @pl.when((at >= 1) & (at < CHIPS + 1))
        def _():
            cross(at - 1).start()

        @pl.when((at >= hand_lag) & (at < CHIPS + hand_lag))
        def _():
            for which in range(CORES):
                target, away, keep = hand(at - hand_lag, which)

                @pl.when(target != tok)
                def _():
                    away.start()

                @pl.when(target == tok)
                def _():
                    keep.start()

        @pl.when(at < CHIPS)
        def _():
            query(at)

        @pl.when(at == CHIPS)
        def _():
            for copy in later:
                copy.wait()
            key()

        @pl.when((at >= sum_lag) & (at < CHIPS + sum_lag))
        def _():
            done = at - sum_lag
            cross(done).wait_recv()
            sum_buf[done] = (own_buf[done] + part_recv[done].astype(jnp.float32)).astype(sum_buf.dtype)

    loop(CHIPS + hand_lag, body)

    def drain(at):
        cross(at).wait_send()
        for which in range(CORES):
            target, away, keep = hand(at, which)

            @pl.when(target != tok)
            def _():
                away.wait_send()

            @pl.when(target == tok)
            def _():
                keep.wait()

    loop(CHIPS, drain)
    others = heads.at[pl.ds(0, groups - 1)]
    pltpu.make_async_remote_copy(
        src_ref=others, dst_ref=others, send_sem=sum_sem.at[0, 0], recv_sem=head_sem.at[0],
        device_id=(tok, partner), device_id_type=MESH,
    ).wait_recv()


Q_TILE = 1024


def finish(gathered, slots, other, normed):
    features, head = other.shape
    groups = CHIPS * CORES
    rows = gathered.shape[0] // CHIPS
    block = rows // CORES
    depth = slots.shape[1]
    kind, wide = gathered.dtype, jnp.float32
    any_space = pl.BlockSpec(memory_space=pl.ANY)
    vmem = pl.BlockSpec(memory_space=pltpu.VMEM)
    return pl.pallas_call(
        finish_kernel,
        out_shape=(
            jax.ShapeDtypeStruct((groups, block, head), kind),
            jax.ShapeDtypeStruct((block, CORES * head), wide),
        ),
        in_specs=[any_space] * 4,
        out_specs=(any_space, vmem),
        scratch_shapes=[
            pltpu.VMEM((features, 2 * head), kind),
            pltpu.VMEM((2, rows, features), kind),
            pltpu.VMEM((block, depth), kind),
            pltpu.VMEM((depth, CORES * head), kind),
            pltpu.VMEM((rows, 2 * head), wide),
            pltpu.VMEM((CHIPS, rows, head), wide),
            pltpu.VMEM((CHIPS, rows, head), kind),
            pltpu.VMEM((CHIPS, rows, head), kind),
            pltpu.VMEM((CHIPS, rows, head), kind),
            pltpu.SemaphoreType.DMA((2,)),
            pltpu.SemaphoreType.DMA((3 + CORES,)),
            pltpu.SemaphoreType.DMA((2, CHIPS)),
            pltpu.SemaphoreType.DMA((CHIPS, CORES)),
            pltpu.SemaphoreType.DMA((1,)),
            pltpu.SemaphoreType.DMA((1,)),
        ],
        compiler_params=pltpu.CompilerParams(collective_id=groups, has_side_effects=True),
    )(gathered, slots, other, normed)


def output_kernel(scale, gram_ref, heads_ref, raw_ref, cos_ref, sin_ref, hess_ref, q_ref, k_ref):
    count, block, head = heads_ref.shape
    even = lax.broadcasted_iota(jnp.int32, (block, head), 1) % 2 == 0

    def turned(raw):
        swapped = jnp.where(even, pltpu.roll(raw, head - 1, 1), pltpu.roll(raw, 1, 1))
        return raw * cos_ref[...] + swapped * sin_ref[...]

    hess_ref[...] = gram_ref[...] * scale
    for at in range(count):
        q_ref[:, at * head : (at + 1) * head] = turned(heads_ref[at].astype(jnp.float32)).astype(q_ref.dtype)

    @pl.when(pl.program_id(0) == 0)
    def _():
        for at in range(k_ref.shape[1] // head):
            lanes = slice(at * head, (at + 1) * head)
            k_ref[:, lanes] = turned(raw_ref[:, lanes]).astype(k_ref.dtype)


def outputs(scale, gram, heads, raw, cosine, sine):
    rows, columns = gram.shape
    groups, block, head = heads.shape
    pieces = CHIPS
    whole = lambda array: pl.BlockSpec(array.shape, lambda at: (0,) * array.ndim)
    return pl.pallas_call(
        functools.partial(output_kernel, scale),
        grid=(pieces,),
        out_shape=(
            jax.ShapeDtypeStruct(gram.shape, gram.dtype),
            jax.ShapeDtypeStruct((block, groups * head), heads.dtype),
            jax.ShapeDtypeStruct(raw.shape, heads.dtype),
        ),
        in_specs=[
            pl.BlockSpec((rows // pieces, columns), lambda at: (at, 0)),
            pl.BlockSpec((groups // pieces, block, head), lambda at: (at, 0, 0)),
            whole(raw), whole(cosine), whole(sine),
        ],
        out_specs=(
            pl.BlockSpec((rows // pieces, columns), lambda at: (at, 0)),
            pl.BlockSpec((block, groups // pieces * head), lambda at: (0, at)),
            whole(raw),
        ),
    )(gram, heads, raw, cosine, sine)


def angles(place):
    dims = jnp.arange(HEAD, dtype=jnp.int32)
    pair = (dims // 2).astype(jnp.float32)
    freq = jnp.power(jnp.float32(rope_base), -2.0 * pair / HEAD)
    angle = place.astype(jnp.float32)[:, None] * freq[None, :]
    sine = jnp.where((dims % 2 == 0)[None, :], -jnp.sin(angle), jnp.sin(angle))
    return jnp.cos(angle), sine


def grid_shards(hidden, norm_gain, token_ids, owner, query_store, key_store):
    cosine, sine = lax.optimization_barrier(angles(positions(token_ids)))
    groups = lax.axis_size("tok")
    branches = [functools.partial(exchange, at) for at in range(groups)]
    gathered, slots, other, normed, gram = lax.switch(owner[0], branches, hidden, norm_gain[None, :], query_store, key_store)
    heads, raw_k = finish(gathered, slots, other, normed)
    scale = 2.0 / (hidden.shape[0] * groups)
    hessian, queries, keys = outputs(scale, gram, heads, raw_k, cosine, sine)
    return (queries, keys, hessian)


def solution(mesh):
    placed = (P("tok", None), P(), P("tok"), P(), P("tok", None, "col"), P("tok", None, "col"))
    fits = mesh.shape["tok"] == CHIPS * CORES and mesh.shape["col"] == 2
    return jax.shard_map(
        grid_shards if fits else shards,
        mesh=mesh,
        in_specs=placed,
        out_specs=(P("tok", "col"), P("tok", "col"), P("col", "tok")),
        check_vma=False,
    )
```
